32 devices in a mesh: dp: 4 (over x, core), ctx: 2 (over y), head: 4 (over z).
Axes of the slice: x: 2, y: 2, z: 4, core: 2. Of those that a mesh axis runs over, the one named last changes fastest.
Arguments:
- latent: bfloat16 [4, 256, 512], P('dp', 'ctx'), may hold values from -6 to 6
- rope: bfloat16 [4, 256, 64], P('dp', 'ctx'), may hold values from -6 to 6
- query: bfloat16 [4, 256, 12288], P('dp', 'ctx', 'head'), may hold values from -9 to 9
- grad_out: bfloat16 [4, 256, 8192], P('dp', 'ctx', 'head'), may hold values from -6 to 6
- attn_out: bfloat16 [4, 256, 8192], P('dp', 'ctx', 'head'), may hold values from -40 to 40
- lse: float32 [4, 64, 256], P('dp', 'head', 'ctx'), may hold values from -100 to 100, as said below
- positions: int32 [4, 256], P('dp'), may hold values from 0 to 255, as said below
- w_uk: bfloat16 [512, 8192], P(None, 'head'), may hold values from -2 to 2
- w_uv: bfloat16 [512, 8192], P(None, 'head'), may hold values from -2 to 2
Outputs:
- grad_query: bfloat16 [4, 256, 12288], P('dp', 'ctx', 'head')
- grad_latent: float32 [4, 256, 512], P('dp', 'ctx')
- grad_rope: float32 [4, 256, 64], P('dp', 'ctx')
- grad_wuk: bfloat16 [512, 8192], P(('dp', 'ctx'), 'head')
- grad_wuv: bfloat16 [512, 8192], P(('dp', 'ctx'), 'head')
The draws below stay inside these ranges and needn't reach their ends.
Inputs may be any that keep to these rules, and one draw needn't show every extreme that they name: Each sequence's row is a permutation of 0 to 255 made of runs of 64 consecutive positions, each run filling an aligned run of 64 rows in rising order; which run goes to which rows is drawn. lse[h, i] is the log of the sum of exp(scores[i, j]) over the keys j with positions[j] <= positions[i].
All inputs are finite; a program needn't handle non-finite values.
Results may differ from the reference program's by a relative error of at most 0.02.
Values may be sent and summed in bfloat16 or wider, within the bound.
No kernel may reach another device: no remote copies, remote signals or barrier semaphores. Data moves between devices by JAX's collectives and lax.ppermute only.
A program may use at most 64 MiB of HBM per device.

```python
import math
import jax
import jax.numpy as jnp
from jax import lax

DL = 512
DR = 64
DN = 128
DV = 128
HEADS = 64
HALF = 64
TOKENS = 256
SEQS = 4


MASKED = -1e+30


def draw_order(key):
    block_count = TOKENS // HALF

    def one_sequence(index):
        shuffled = jax.random.permutation(jax.random.fold_in(key, 5000 + index), block_count).astype(jnp.int32)
        token_index = jnp.arange(TOKENS, dtype=jnp.int32)
        return (shuffled[token_index // HALF] * HALF + token_index % HALF).astype(jnp.int32)
    return jax.vmap(one_sequence)(jnp.arange(SEQS, dtype=jnp.int32))


def make_floats(key):
    streams = [jax.random.fold_in(key, 900 + index) for index in range(8)]
    latent = jnp.clip(jax.random.normal(streams[0], (SEQS, TOKENS, DL), jnp.float32), -6.0, 6.0)
    query = jnp.clip(1.4 * jax.random.normal(streams[2], (SEQS, TOKENS, HEADS * (DN + DR)), jnp.float32), -8.0, 8.0)
    grad_out = jnp.clip(jax.random.normal(streams[5], (SEQS, TOKENS, HEADS * DV), jnp.float32), -6.0, 6.0)
    rope = jnp.clip(jax.random.normal(streams[1], (SEQS, TOKENS, DR), jnp.float32), -6.0, 6.0)
    w_uk = jnp.clip(jax.random.normal(streams[3], (DL, HEADS * DN), jnp.float32), -6.0, 6.0) / math.sqrt(DL)
    w_uv = jnp.clip(jax.random.normal(streams[4], (DL, HEADS * DV), jnp.float32), -6.0, 6.0) / math.sqrt(DL)
    return (latent.astype(jnp.bfloat16), rope.astype(jnp.bfloat16), query.astype(jnp.bfloat16), grad_out.astype(jnp.bfloat16), w_uk.astype(jnp.bfloat16), w_uv.astype(jnp.bfloat16))


def forward_pass(key):
    latent, rope, query, grad_out, w_uk, w_uv = make_floats(key)
    seq_orders = draw_order(jax.random.fold_in(key, 77))
    score_scale = 1.0 / math.sqrt(DN + DR)

    def one_sequence(item):
        seq_latent, seq_rope, seq_query, seq_order = item
        nope = jnp.dot(seq_latent, w_uk, preferred_element_type=jnp.float32).astype(jnp.bfloat16)
        nope = nope.reshape(TOKENS, HEADS, DN).transpose(1, 0, 2)
        value_rows = jnp.dot(seq_latent, w_uv, preferred_element_type=jnp.float32).astype(jnp.bfloat16)
        value_rows = value_rows.reshape(TOKENS, HEADS, DV).transpose(1, 0, 2)
        queries = seq_query.reshape(TOKENS, HEADS, DN + DR).transpose(1, 0, 2)
        allowed = seq_order[None, :] <= seq_order[:, None]

        def one_head(part_item):
            head_query, head_nope, head_values = part_item
            head_keys = jnp.concatenate([head_nope, seq_rope], axis=1)
            scores = jnp.dot(head_query, head_keys.T, preferred_element_type=jnp.float32) * score_scale
            scores = jnp.where(allowed, scores, MASKED)
            top_score = jnp.max(scores, axis=1, keepdims=True)
            expo = jnp.exp(scores - top_score)
            total = jnp.sum(expo, axis=1, keepdims=True)
            mixed = jnp.dot(expo / total, head_values.astype(jnp.float32), precision=lax.Precision.HIGHEST)
            return (mixed, top_score[:, 0] + jnp.log(total[:, 0]))
        mixed, log_total = lax.map(one_head, (queries, nope, value_rows))
        return (mixed.transpose(1, 0, 2).reshape(TOKENS, HEADS * DV), log_total)
    return lax.map(one_sequence, (latent, rope, query, seq_orders))


def draw_latent(key, part):
    return make_floats(key)[0]


def draw_rope(key, part):
    return make_floats(key)[1]


def draw_query(key, part):
    return make_floats(key)[2]


def draw_grad_out(key, part):
    return make_floats(key)[3]


def draw_w_uk(key, part):
    return make_floats(key)[4]


def draw_w_uv(key, part):
    return make_floats(key)[5]


def draw_attn_out(key, part):
    return forward_pass(key)[0].astype(jnp.bfloat16)


def draw_lse(key, part):
    return forward_pass(key)[1].astype(jnp.float32)


def draw_positions(key, part):
    return draw_order(jax.random.fold_in(key, 77))


def setup_inputs(seed: int = 0) -> dict:
    streams_of = jax.random.split(jax.random.key(seed), 10)
    return {
        "latent": draw_latent(jax.random.fold_in(streams_of[9], 71), 0),
        "rope": draw_rope(jax.random.fold_in(streams_of[9], 71), 0),
        "query": draw_query(jax.random.fold_in(streams_of[9], 71), 0),
        "grad_out": draw_grad_out(jax.random.fold_in(streams_of[9], 71), 0),
        "attn_out": draw_attn_out(jax.random.fold_in(streams_of[9], 71), 0),
        "lse": draw_lse(jax.random.fold_in(streams_of[9], 71), 0),
        "positions": draw_positions(jax.random.fold_in(streams_of[9], 71), 0),
        "w_uk": draw_w_uk(jax.random.fold_in(streams_of[9], 71), 0),
        "w_uv": draw_w_uv(jax.random.fold_in(streams_of[9], 71), 0),
    }


MASKED = -1e+30

def sequence_grads(latent, rope, query, grad_out, attn_out, lse, positions, w_uk, w_uv):
    score_scale = 1.0 / math.sqrt(DN + DR)
    keys_nope = jnp.dot(latent, w_uk, preferred_element_type=jnp.float32).astype(jnp.bfloat16)
    keys_nope = keys_nope.reshape(TOKENS, HEADS, DN).transpose(1, 0, 2)
    values = jnp.dot(latent, w_uv, preferred_element_type=jnp.float32).astype(jnp.bfloat16)
    values = values.reshape(TOKENS, HEADS, DV).transpose(1, 0, 2)
    queries = query.reshape(TOKENS, HEADS, DN + DR).transpose(1, 0, 2)
    grads = grad_out.reshape(TOKENS, HEADS, DV).transpose(1, 0, 2)
    outputs = attn_out.reshape(TOKENS, HEADS, DV).transpose(1, 0, 2)
    allowed = positions[None, :] <= positions[:, None]

    def per_head(item):
        head_query, head_nope, head_values, head_grads, head_outputs, head_lse = item
        head_keys = jnp.concatenate([head_nope, rope], axis=1)
        scores = jnp.dot(head_query, head_keys.T, preferred_element_type=jnp.float32) * score_scale
        weights = jnp.exp(jnp.where(allowed, scores - head_lse[:, None], MASKED))
        dots = jnp.dot(head_grads, head_values.T, preferred_element_type=jnp.float32)
        delta = lax.optimization_barrier(jnp.sum(head_grads.astype(jnp.float32) * head_outputs.astype(jnp.float32), axis=1))
        score_grad = (weights * (dots - delta[:, None]) * score_scale).astype(jnp.bfloat16)
        weights_b = weights.astype(jnp.bfloat16)
        query_grad = jnp.dot(score_grad, head_keys, preferred_element_type=jnp.float32)
        key_grad = jnp.dot(score_grad.T, head_query, preferred_element_type=jnp.float32)
        value_grad = jnp.dot(weights_b.T, head_grads, preferred_element_type=jnp.float32)
        return (query_grad, key_grad, value_grad)
    query_grad, key_grad, value_grad = lax.map(per_head, (queries, keys_nope, values, grads, outputs, lse))
    query_out = query_grad.transpose(1, 0, 2).reshape(TOKENS, HEADS * (DN + DR)).astype(jnp.bfloat16)
    key_nope = key_grad[:, :, :DN].transpose(1, 0, 2).reshape(TOKENS, HEADS * DN)
    value_flat = value_grad.transpose(1, 0, 2).reshape(TOKENS, HEADS * DV)
    rope_grad = lax.optimization_barrier(jnp.sum(key_grad[:, :, DN:], axis=0))
    highest = lax.Precision.HIGHEST
    latent_grad = jnp.dot(key_nope, w_uk.astype(jnp.float32).T, precision=highest) + jnp.dot(value_flat, w_uv.astype(jnp.float32).T, precision=highest)
    latent_f = latent.astype(jnp.float32).T
    weight_uk = jnp.dot(latent_f, key_nope, precision=highest)
    weight_uv = jnp.dot(latent_f, value_flat, precision=highest)
    return (query_out, latent_grad, rope_grad, weight_uk, weight_uv)

def reference(latent, rope, query, grad_out, attn_out, lse, positions, w_uk, w_uv):

    def one_sequence(totals, item):
        seq_latent, seq_rope, seq_query, seq_grads, seq_outputs, seq_lse, seq_order = item
        query_out, latent_grad, rope_grad, weight_uk, weight_uv = sequence_grads(seq_latent, seq_rope, seq_query, seq_grads, seq_outputs, seq_lse, seq_order, w_uk, w_uv)
        return ((totals[0] + weight_uk, totals[1] + weight_uv), (query_out, latent_grad, rope_grad))
    initial = (jnp.zeros((DL, HEADS * DN), jnp.float32), jnp.zeros((DL, HEADS * DV), jnp.float32))
    totals, stacked = lax.scan(one_sequence, initial, (latent, rope, query, grad_out, attn_out, lse, positions))
    return (stacked[0], stacked[1], stacked[2], totals[0].astype(jnp.bfloat16), totals[1].astype(jnp.bfloat16))
```

```python
import functools
import math

import jax
import jax.numpy as jnp
import numpy as np
from jax import lax
from jax.experimental import pallas as pl
from jax.experimental.pallas import tpu as pltpu
from jax.sharding import PartitionSpec as P

DR = 64
DN = 128
DV = 128
DQ = DN + DR

MASKED = -1e30
NT = (((1,), (1,)), ((), ()))


def bits_of(count):
    return [1 << b for b in range(count.bit_length() - 1)]


def stage_orders(dp_size, ctx_size):
    outer = [("dp", bit) for bit in bits_of(dp_size)[1:]]
    inner = [("ctx", bit) for bit in bits_of(ctx_size)]
    return outer + inner, inner + outer


def row_table(dp_size, ctx_size, rows):
    orders = stage_orders(dp_size, ctx_size)
    blocks = dp_size * ctx_size
    width = rows // blocks
    table = np.zeros((blocks, rows), np.int32)
    for dp in range(dp_size):
        for ctx in range(ctx_size):
            for place in range(blocks):
                digits = [(place >> b) & 1 for b in reversed(range(blocks.bit_length() - 1))]
                target = {"dp": dp, "ctx": ctx}
                if digits[0] == 0:
                    target["dp"] ^= 1
                for digit, (axis, bit) in zip(digits[1:], orders[target["dp"] & 1]):
                    if digit == 0:
                        target[axis] ^= bit
                block = target["dp"] * ctx_size + target["ctx"]
                table[dp * ctx_size + ctx, place * width:(place + 1) * width] = (
                    block * width + np.arange(width)
                )
    return table


def stage_pairs(stage, dp_size, ctx_size):
    pairs = []
    orders = stage_orders(dp_size, ctx_size)
    for dp in range(dp_size):
        for ctx in range(ctx_size):
            place = {"dp": dp, "ctx": ctx}
            axis, bit = ("dp", 1) if stage == 0 else orders[dp & 1][stage - 1]
            place[axis] ^= bit
            pairs.append((dp * ctx_size + ctx, place["dp"] * ctx_size + place["ctx"]))
    return pairs


def dot(a, b):
    return jnp.dot(a, b, preferred_element_type=jnp.float32)


def dot_nt(a, b):
    return lax.dot_general(a, b, NT, preferred_element_type=jnp.float32)


def grads_body(place_ref, pos_ref, order_ref, latent_ref, rope_ref, query_ref, grad_ref, out_ref,
               lse_ref, wuk_ref, wuv_ref, *rest, heads, chunk_start, has_prior, final):
    if has_prior:
        prior_ref, _, *rest = rest
    dq_ref, send_ref, keep_ref, total_ref, flat_ref, bias_ref, acc_ref, rope_acc_ref = rest
    step = pl.program_id(0)
    steps = pl.num_programs(0)
    tokens = latent_ref.shape[0]
    rows = query_ref.shape[0]
    scale = 1.0 / math.sqrt(DQ)
    latent = latent_ref[...]
    rope = rope_ref[...]

    @pl.when(step == 0)
    def _():
        width = latent_ref.shape[1]
        spot = lax.broadcasted_iota(jnp.int32, (width, width), 0)
        pick = jnp.where(spot == order_ref[0], 1.0, 0.0).astype(jnp.bfloat16)
        flat_ref[...] = dot(latent, pick).T.astype(jnp.bfloat16)
        mine = place_ref[1]
        count = tokens // rows
        own_pos = pos_ref[mine]
        for chunk in range(count):
            key_pos = pos_ref[lax.rem(mine + chunk, count)]
            key_col = jnp.broadcast_to(key_pos, (rows, rows)).T
            bias_ref[chunk * rows:(chunk + 1) * rows, :] = jnp.where(
                key_col <= jnp.broadcast_to(own_pos, (rows, rows)), 0.0, MASKED
            )
        if has_prior:
            acc_ref[...] = prior_ref[:, :width]
            rope_acc_ref[...] = prior_ref[:, width:]
        else:
            acc_ref[...] = jnp.zeros_like(acc_ref)
            rope_acc_ref[...] = jnp.zeros_like(rope_acc_ref)

    bias = bias_ref[...]
    key_grads = []
    value_grads = []
    rope_total = rope_acc_ref[...]
    for head in range(heads):
        cols = slice(head * DN, (head + 1) * DN)
        wide = slice(head * DQ, (head + 1) * DQ)
        keys = jnp.concatenate([dot(latent, wuk_ref[:, cols]).astype(jnp.bfloat16), rope], axis=1)
        values = dot(latent, wuv_ref[:, cols]).astype(jnp.bfloat16)
        query = query_ref[:, wide]
        grad = grad_ref[:, cols]
        product = grad.astype(jnp.float32) * out_ref[:, cols].astype(jnp.float32)
        delta = jnp.sum(product.T, axis=0, keepdims=True)
        lse = lse_ref[pl.ds((chunk_start + step) * heads + head, 1), :]
        weights = jnp.exp(dot_nt(keys, query) * scale - lse + bias)
        score_grad = (weights * (dot_nt(values, grad) - delta) * scale).astype(jnp.bfloat16)
        dq_ref[:, wide] = dot(score_grad.T, keys).astype(jnp.bfloat16)
        key_grad = dot(score_grad, query)
        value_grads.append(dot(weights.astype(jnp.bfloat16), grad).astype(jnp.bfloat16))
        key_grads.append(key_grad[:, :DN].astype(jnp.bfloat16))
        rope_total = rope_total + key_grad[:, DN:]
    rope_acc_ref[...] = rope_total
    key_flat = jnp.concatenate(key_grads, axis=1)
    value_flat = jnp.concatenate(value_grads, axis=1)
    half = flat_ref.shape[0] // 2
    flat = flat_ref[...]
    weight_uk = dot(flat, key_flat).astype(jnp.bfloat16)
    weight_uv = dot(flat, value_flat).astype(jnp.bfloat16)
    send_ref[0] = weight_uk[:half]
    send_ref[1] = weight_uv[:half]
    keep_ref[0] = weight_uk[half:]
    keep_ref[1] = weight_uv[half:]
    acc_ref[...] += dot_nt(key_flat, wuk_ref[...]) + dot_nt(value_flat, wuv_ref[...])

    @pl.when(step == steps - 1)
    def _():
        width = latent_ref.shape[1]
        total_ref[:, :width] = acc_ref[...].astype(total_ref.dtype)
        total_ref[:, width:] = rope_acc_ref[...].astype(total_ref.dtype)


def chunk_grads(place, positions, order, latent, rope, query, grad_out, attn_out, lse, w_uk, w_uv,
                prior, *, chunk, chunks, heads):
    tokens, width = latent.shape
    rows = query.shape[0]
    head_count = lse.shape[0]
    steps = head_count // heads // chunks
    start = chunk * steps
    final = chunk + 1 == chunks
    whole = lambda shape: pl.BlockSpec(shape, lambda j, p: (0,) * len(shape))
    columns = lambda height, size: pl.BlockSpec((height, size), lambda j, p: (0, start + j))
    in_specs = [
        whole(positions.shape),
        pl.BlockSpec((1, 1, width), lambda j, p: (p[0], 0, 0)),
        whole(latent.shape),
        whole(rope.shape),
        columns(rows, heads * DQ),
        columns(rows, heads * DV),
        columns(rows, heads * DV),
        whole(lse.shape),
        columns(width, heads * DN),
        columns(width, heads * DV),
    ]
    operands = [positions, order, latent, rope, query, grad_out, attn_out, lse, w_uk, w_uv]
    aliases = {}
    if prior is not None:
        in_specs += [whole(prior[1].shape), pl.BlockSpec(memory_space=pl.ANY)]
        operands += [prior[1], prior[0]]
        aliases = {len(operands): 0}
    half = jax.ShapeDtypeStruct((2, width // 2, steps * heads * DN), jnp.bfloat16)
    half_spec = pl.BlockSpec((2, width // 2, heads * DN), lambda j, p: (0, 0, j))
    total = jax.ShapeDtypeStruct((tokens, width + DR), jnp.bfloat16 if final else jnp.float32)
    return pl.pallas_call(
        functools.partial(grads_body, heads=heads, chunk_start=start,
                          has_prior=prior is not None, final=final),
        grid_spec=pltpu.PrefetchScalarGridSpec(
            num_scalar_prefetch=1,
            grid=(steps,),
            in_specs=in_specs,
            out_specs=[columns(rows, heads * DQ), half_spec, half_spec, whole(total.shape)],
            scratch_shapes=[
                pltpu.VMEM((width, tokens), jnp.bfloat16),
                pltpu.VMEM((tokens, rows), jnp.float32),
                pltpu.VMEM((tokens, width), jnp.float32),
                pltpu.VMEM((tokens, DR), jnp.float32),
            ],
        ),
        out_shape=[jax.ShapeDtypeStruct(query.shape, jnp.bfloat16), half, half, total],
        input_output_aliases=aliases,
        name="grads",
    )(place, *operands)


def shifted(value, axis, steps):
    count = lax.axis_size(axis)
    return lax.ppermute(value, axis, [(s, (s + steps) % count) for s in range(count)])


def on_device(latent, rope, query, grad_out, attn_out, lse, positions, w_uk, w_uv):
    dp_size, ctx_size, head_size = (lax.axis_size(a) for a in ("dp", "ctx", "head"))
    rows, width = latent.shape[1:]
    my_ctx = lax.axis_index("ctx")
    my_place = lax.axis_index("dp") * ctx_size + my_ctx
    place = jnp.stack([my_place, my_ctx]).astype(jnp.int32)
    order = jnp.asarray(row_table(dp_size, ctx_size, width))[:, None, :]
    own = jnp.concatenate([latent[0], rope[0]], axis=1)
    features = jnp.concatenate([own] + [shifted(own, "ctx", -s) for s in range(1, ctx_size)], axis=0)
    head_count = lse.shape[1]
    heads = math.gcd(head_count, 4)
    chunks = math.gcd(head_count // heads, 2)
    prior = None
    sends = []
    keeps = []
    for chunk in range(chunks):
        grad_query, send, keep, total = chunk_grads(
            place, positions.reshape(ctx_size, 1, rows), order, features[:, :width],
            features[:, width:], query[0], grad_out[0], attn_out[0], lse[0], w_uk, w_uv, prior,
            chunk=chunk, chunks=chunks, heads=heads,
        )
        prior = (grad_query, total)
        sends.append(send)
        keeps.append(keep)
    parts = total.reshape(ctx_size, rows, width + DR)
    summed = parts[0].astype(jnp.float32)
    for s in range(1, ctx_size):
        summed = summed + shifted(parts[s], "ctx", s).astype(jnp.float32)
    for bit in bits_of(head_size):
        mine = summed.astype(jnp.bfloat16)
        other = lax.ppermute(mine, "head", [(s, s ^ bit) for s in range(head_size)])
        summed = mine.astype(jnp.float32) + other.astype(jnp.float32)
    stages = (dp_size * ctx_size).bit_length() - 1
    finals = []
    for send, keep in zip(sends, keeps):
        for stage in range(stages):
            got = lax.ppermute(send, ("dp", "ctx"), stage_pairs(stage, dp_size, ctx_size))
            left = keep.astype(jnp.float32) + got.astype(jnp.float32)
            left = left.astype(jnp.bfloat16)
            half = left.shape[1] // 2
            send, keep = left[:, :half], left[:, half:]
        finals.append(left)
    weight_uk = jnp.concatenate([part[0] for part in finals], axis=1)
    weight_uv = jnp.concatenate([part[1] for part in finals], axis=1)
    return (
        grad_query[None],
        summed[None, :, :width],
        summed[None, :, width:],
        weight_uk,
        weight_uv,
    )


def solution(mesh):
    return jax.shard_map(
        on_device,
        mesh=mesh,
        in_specs=(
            P("dp", "ctx", None),
            P("dp", "ctx", None),
            P("dp", "ctx", "head"),
            P("dp", "ctx", "head"),
            P("dp", "ctx", "head"),
            P("dp", "head", "ctx"),
            P("dp", None),
            P(None, "head"),
            P(None, "head"),
        ),
        out_specs=(
            P("dp", "ctx", "head"),
            P("dp", "ctx", None),
            P("dp", "ctx", None),
            P(("dp", "ctx"), "head"),
            P(("dp", "ctx"), "head"),
        ),
        check_vma=False,
    )
```

```python
import functools
import math

import jax
import jax.numpy as jnp
import numpy as np
from jax import lax
from jax.experimental import pallas as pl
from jax.experimental.pallas import tpu as pltpu
from jax.sharding import PartitionSpec as P

DR = 64
DN = 128
DV = 128
DQ = DN + DR

MASKED = -1e30
GROUP = 4
VMEM_LIMIT = 16 << 20
LOAD_LIMIT = 16 << 20
CHUNKS = 2
NT = (((1,), (1,)), ((), ()))


def bits_of(count):
    return [1 << b for b in range(count.bit_length() - 1)]


def stage_orders(dp_size, ctx_size):
    outer = [("dp", bit) for bit in bits_of(dp_size)[1:]]
    inner = [("ctx", bit) for bit in bits_of(ctx_size)]
    return outer + inner, inner + outer


def row_table(dp_size, ctx_size, rows):
    orders = stage_orders(dp_size, ctx_size)
    blocks = dp_size * ctx_size
    width = rows // blocks
    table = np.zeros((blocks, rows), np.int32)
    for dp in range(dp_size):
        for ctx in range(ctx_size):
            for place in range(blocks):
                digits = [(place >> b) & 1 for b in reversed(range(blocks.bit_length() - 1))]
                target = {"dp": dp, "ctx": ctx}
                if digits[0] == 0:
                    target["dp"] ^= 1
                for digit, (axis, bit) in zip(digits[1:], orders[target["dp"] & 1]):
                    if digit == 0:
                        target[axis] ^= bit
                block = target["dp"] * ctx_size + target["ctx"]
                table[dp * ctx_size + ctx, place * width:(place + 1) * width] = (
                    block * width + np.arange(width)
                )
    return table


def stage_pairs(stage, dp_size, ctx_size):
    pairs = []
    orders = stage_orders(dp_size, ctx_size)
    for dp in range(dp_size):
        for ctx in range(ctx_size):
            place = {"dp": dp, "ctx": ctx}
            axis, bit = ("dp", 1) if stage == 0 else orders[dp & 1][stage - 1]
            place[axis] ^= bit
            pairs.append((dp * ctx_size + ctx, place["dp"] * ctx_size + place["ctx"]))
    return pairs


def dot(a, b):
    return jnp.dot(a, b, preferred_element_type=jnp.float32)


def dot_nt(a, b):
    return lax.dot_general(a, b, NT, preferred_element_type=jnp.float32)


def load_body(place_ref, pos_ref, order_ref, latent_ref, rope_ref, query_ref, grad_ref, out_ref,
              lse_ref, wuk_ref, wuv_ref, latent_out, rope_out, query_out, grad_out, lse_out,
              delta_out, wuk_out, wuv_out, keys_out, values_out, flat_out, bias_out,
              pos, order, attn, sems, *, ctx_size):
    pairs = [(latent_ref, latent_out), (order_ref, order), (pos_ref, pos), (rope_ref, rope_out),
             (wuk_ref, wuk_out), (wuv_ref, wuv_out), (grad_ref, grad_out), (out_ref, attn),
             (lse_ref, lse_out), (query_ref, query_out)]
    copies = [pltpu.make_async_copy(a, b, sems.at[k]) for k, (a, b) in enumerate(pairs)]
    for copy in copies:
        copy.start()
    rows, width = latent_out.shape
    for copy in copies[:3]:
        copy.wait()
    mine = place_ref[1]
    own_pos = jnp.broadcast_to(pos[mine], (rows, rows))
    for chunk in range(ctx_size):
        key_pos = pos[lax.rem(mine + chunk, ctx_size)]
        key_col = jnp.broadcast_to(key_pos, (rows, rows)).T
        bias_out[chunk * rows:(chunk + 1) * rows, :] = jnp.where(key_col <= own_pos, 0.0, MASKED)
    latent = latent_out[...]
    flat_out[...] = rows_first(latent, order[place_ref[0]])
    copies[4].wait()
    keys_out[...] = dot(latent, wuk_out[...]).astype(jnp.bfloat16)
    copies[5].wait()
    values_out[...] = dot(latent, wuv_out[...]).astype(jnp.bfloat16)
    copies[6].wait()
    copies[7].wait()
    for head in range(delta_out.shape[0]):
        cols = slice(head * DV, (head + 1) * DV)
        product = grad_out[:, cols].astype(jnp.float32) * attn[:, cols].astype(jnp.float32)
        delta_out[head:head + 1, :] = jnp.sum(product.T, axis=0, keepdims=True)
    for k in (3, 8, 9):
        copies[k].wait()


def rows_first(latent, order):
    width = latent.shape[1]
    spot = lax.broadcasted_iota(jnp.int32, (width, width), 0)
    pick = jnp.where(spot == order, 1.0, 0.0).astype(jnp.bfloat16)
    return dot(latent, pick).astype(jnp.bfloat16).T


def grads_body(place_ref, order_ref, *rest, ctx_size, start, count, group, has_prior, final, pieces):
    far_latents = rest[:ctx_size - 1]
    far_ropes = rest[ctx_size - 1:2 * ctx_size - 2]
    (latent_ref, rope_ref, query_ref, grad_ref, lse_ref, delta_ref, wuk_ref, wuv_ref, keys_ref,
     values_ref, flat_ref, bias_ref, *rest) = rest[2 * ctx_size - 2:]
    if has_prior:
        prior_ref, *rest = rest
    dq_ref, *rest = rest
    piece_refs, total_refs = rest[:pieces], rest[pieces:]
    rows, width = latent_ref.shape
    scale = 1.0 / math.sqrt(DQ)
    rope = jnp.concatenate([ref[...] for ref in (rope_ref, *far_ropes)], axis=1).T
    far = jnp.concatenate([ref[...] for ref in far_latents], axis=0)
    bias = bias_ref[...]
    flat = jnp.concatenate([flat_ref[...], rows_first(far, order_ref[place_ref[0]])], axis=1)
    rope_total = prior_ref[:, width:] if has_prior else 0.0
    latent_total = prior_ref[:, :width] if has_prior else 0.0
    for first in range(0, count, group):
        span = slice((start + first) * DN, (start + first + group) * DN)
        out_span = slice(first * DN, (first + group) * DN)
        wuk = wuk_ref[:, span]
        wuv = wuv_ref[:, span]
        keys_all = jnp.concatenate([keys_ref[:, span], dot(far, wuk).astype(jnp.bfloat16)], axis=0)
        values_all = jnp.concatenate(
            [values_ref[:, span], dot(far, wuv).astype(jnp.bfloat16)], axis=0
        )
        key_grads = []
        value_grads = []
        for inner in range(group):
            head = start + first + inner
            cols = slice(head * DN, (head + 1) * DN)
            wide = slice(head * DQ, (head + 1) * DQ)
            out_wide = slice((first + inner) * DQ, (first + inner + 1) * DQ)
            part = slice(inner * DN, (inner + 1) * DN)
            keys = jnp.concatenate([keys_all[:, part], rope], axis=1)
            query = query_ref[:, wide]
            grad = grad_ref[:, cols]
            delta = delta_ref[head:head + 1, :]
            lse = lse_ref[head:head + 1, :]
            weights = jnp.exp(dot_nt(keys, query) * scale - lse + bias)
            dots = dot_nt(values_all[:, part], grad)
            score_grad = (weights * (dots - delta) * scale).astype(jnp.bfloat16)
            dq_ref[:, out_wide] = dot(score_grad.T, keys).astype(jnp.bfloat16)
            key_grad = dot(score_grad, query)
            value_grads.append(dot(weights.astype(jnp.bfloat16), grad).astype(jnp.bfloat16))
            key_grads.append(key_grad[:, :DN].astype(jnp.bfloat16))
            rope_total = rope_total + key_grad[:, DN:]
        key_flat = jnp.concatenate(key_grads, axis=1)
        value_flat = jnp.concatenate(value_grads, axis=1)
        row = 0
        for piece_ref in piece_refs:
            size = piece_ref.shape[1]
            piece_ref[0, :, out_span] = dot(flat[row:row + size], key_flat).astype(jnp.bfloat16)
            piece_ref[1, :, out_span] = dot(flat[row:row + size], value_flat).astype(jnp.bfloat16)
            row += size
        latent_total = latent_total + dot_nt(key_flat, wuk) + dot_nt(value_flat, wuv)
    for chunk, total_ref in enumerate(total_refs):
        part = slice(chunk * rows, chunk * rows + total_ref.shape[0])
        total_ref[:, :width] = latent_total[part].astype(total_ref.dtype)
        total_ref[:, width:] = rope_total[part].astype(total_ref.dtype)


def in_vmem(array):
    return pltpu.with_memory_space_constraint(array, pltpu.VMEM)


def load(place, positions, order, latent, rope, query, grad_out, attn_out, lse, w_uk, w_uv):
    ctx_size = positions.shape[0]
    rows, width = latent.shape
    flat_size = w_uk.shape[1]
    like = lambda a: pltpu.VMEM(a.shape, a.dtype)
    vmem = pl.BlockSpec(memory_space=pltpu.VMEM)
    operands = [positions, order, latent, rope, query, grad_out, attn_out, lse, w_uk, w_uv]
    operands = [pltpu.with_memory_space_constraint(a, pltpu.HBM) for a in operands]
    outs = [like(a) for a in (latent, rope, query, grad_out, lse, lse, w_uk, w_uv)]
    outs += [pltpu.VMEM((rows, flat_size), jnp.bfloat16)] * 2
    outs += [pltpu.VMEM((width, rows), jnp.bfloat16), pltpu.VMEM((ctx_size * rows, rows), jnp.float32)]
    return pl.pallas_call(
        functools.partial(load_body, ctx_size=ctx_size),
        in_specs=[pl.BlockSpec(memory_space=pltpu.SMEM)]
        + [pl.BlockSpec(memory_space=pltpu.HBM)] * len(operands),
        out_specs=[vmem] * len(outs),
        out_shape=outs,
        scratch_shapes=[like(positions), like(order), like(attn_out), pltpu.SemaphoreType.DMA((10,))],
        compiler_params=pltpu.CompilerParams(vmem_limit_bytes=LOAD_LIMIT),
        name="load",
    )(place, *operands)


def chunk_grads(place, order, latents, ropes, loaded, prior, *, start, count, final):
    ctx_size = len(latents) + 1
    rows, width = loaded[0].shape
    blocks = order.shape[0]
    smem = pl.BlockSpec(memory_space=pltpu.SMEM)
    vmem = pl.BlockSpec(memory_space=pltpu.VMEM)
    operands = [*latents, *ropes, *loaded] + ([] if prior is None else [prior])
    operands = [in_vmem(a) for a in operands]
    sizes = [width >> (s + 1) for s in range(blocks.bit_length() - 1)]
    sizes.append(sizes[-1])
    if final:
        totals = [pltpu.VMEM((rows, width + DR), jnp.bfloat16)] * ctx_size
    else:
        totals = [pltpu.VMEM((ctx_size * rows, width + DR), jnp.float32)]
    outs = pl.pallas_call(
        functools.partial(grads_body, ctx_size=ctx_size, start=start, count=count,
                          group=math.gcd(count, GROUP), has_prior=prior is not None, final=final,
                          pieces=len(sizes)),
        in_specs=[smem] + [vmem] * (1 + len(operands)),
        out_specs=[vmem] * (1 + len(sizes) + len(totals)),
        out_shape=[pltpu.VMEM((rows, count * DQ), jnp.bfloat16)]
        + [pltpu.VMEM((2, size, count * DN), jnp.bfloat16) for size in sizes] + totals,
        compiler_params=pltpu.CompilerParams(vmem_limit_bytes=VMEM_LIMIT),
        name="grads",
    )(place, order, *operands)
    return outs[0], outs[1:1 + len(sizes)], outs[1 + len(sizes):]


def shifted(value, axis, steps):
    count = lax.axis_size(axis)
    return lax.ppermute(value, axis, [(s, (s + steps) % count) for s in range(count)])


def on_device(latent, rope, query, grad_out, attn_out, lse, positions, w_uk, w_uv):
    dp_size, ctx_size, head_size = (lax.axis_size(a) for a in ("dp", "ctx", "head"))
    rows, width = latent.shape[1:]
    my_ctx = lax.axis_index("ctx")
    my_place = lax.axis_index("dp") * ctx_size + my_ctx
    place = jnp.stack([my_place, my_ctx]).astype(jnp.int32)
    order = jnp.asarray(row_table(dp_size, ctx_size, width))[:, None, :]
    rope_cols = rope[0].T
    latents = [shifted(latent[0], "ctx", -s) for s in range(1, ctx_size)]
    ropes = [shifted(rope_cols, "ctx", -s) for s in range(1, ctx_size)]
    loaded = load(place, positions.reshape(ctx_size, 1, rows), order, latent[0], rope_cols, query[0],
                  grad_out[0], attn_out[0], lse[0], w_uk, w_uv)
    head_count = lse.shape[1]
    chunks = math.gcd(head_count // math.gcd(head_count, GROUP), CHUNKS)
    count = head_count // chunks
    prior = None
    chunk_pieces = []
    query_grads = []
    for chunk in range(chunks):
        query_grad, pieces, totals = chunk_grads(
            place, order, latents, ropes, loaded, prior,
            start=chunk * count, count=count, final=chunk + 1 == chunks,
        )
        prior = totals[0]
        chunk_pieces.append(pieces)
        query_grads.append(query_grad)
    summed = totals[0].astype(jnp.float32)
    for s in range(1, ctx_size):
        summed = summed + shifted(totals[s], "ctx", s).astype(jnp.float32)
    for bit in bits_of(head_size):
        mine = summed.astype(jnp.bfloat16)
        other = lax.ppermute(mine, "head", [(s, s ^ bit) for s in range(head_size)])
        summed = mine.astype(jnp.float32) + other.astype(jnp.float32)
    finals = []
    for pieces in chunk_pieces:
        arrivals = []
        for stage, piece in enumerate(pieces):
            size = piece.shape[1]
            done = sum(p.shape[1] for p in pieces[:stage])
            value = piece.astype(jnp.float32)
            for past, arrival in enumerate(arrivals):
                first = done - sum(p.shape[1] for p in pieces[:past + 1])
                value = value + arrival[:, first:first + size].astype(jnp.float32)
            value = value.astype(jnp.bfloat16)
            if stage + 1 < len(pieces):
                pairs = stage_pairs(stage, dp_size, ctx_size)
                arrivals.append(lax.ppermute(value, ("dp", "ctx"), pairs))
        finals.append(value)
    weight_uk = jnp.concatenate([part[0] for part in finals], axis=1)
    weight_uv = jnp.concatenate([part[1] for part in finals], axis=1)
    return (
        jnp.concatenate(query_grads, axis=1)[None],
        summed[None, :, :width],
        summed[None, :, width:],
        weight_uk,
        weight_uv,
    )


def solution(mesh):
    return jax.shard_map(
        on_device,
        mesh=mesh,
        in_specs=(
            P("dp", "ctx", None),
            P("dp", "ctx", None),
            P("dp", "ctx", "head"),
            P("dp", "ctx", "head"),
            P("dp", "ctx", "head"),
            P("dp", "head", "ctx"),
            P("dp", None),
            P(None, "head"),
            P(None, "head"),
        ),
        out_specs=(
            P("dp", "ctx", "head"),
            P("dp", "ctx", None),
            P("dp", "ctx", None),
            P(("dp", "ctx"), "head"),
            P(("dp", "ctx"), "head"),
        ),
        check_vma=False,
    )
```

```python
import functools
import math

import jax
import jax.numpy as jnp
import numpy as np
from jax import lax
from jax.experimental import pallas as pl
from jax.experimental.pallas import tpu as pltpu
from jax.sharding import PartitionSpec as P


DR = 64
DN = 128
DV = 128
DQ = DN + DR

MASKED = -1e30
GROUP = 4
VMEM_LIMIT = 6 << 20
LOAD_LIMIT = 4 << 20
ADD_LIMIT = 2 << 20
NT = (((1,), (1,)), ((), ()))


def bits_of(count):
    return [1 << b for b in range(count.bit_length() - 1)]


def stage_orders(dp_size, ctx_size):
    outer = [("dp", bit) for bit in bits_of(dp_size)[1:]]
    inner = [("ctx", bit) for bit in bits_of(ctx_size)]
    return outer + inner, inner + outer


def row_table(dp_size, ctx_size, rows):
    orders = stage_orders(dp_size, ctx_size)
    blocks = dp_size * ctx_size
    width = rows // blocks
    table = np.zeros((blocks, rows), np.int32)
    for dp in range(dp_size):
        for ctx in range(ctx_size):
            for place in range(blocks):
                digits = [(place >> b) & 1 for b in reversed(range(blocks.bit_length() - 1))]
                target = {"dp": dp, "ctx": ctx}
                if digits[0] == 0:
                    target["dp"] ^= 1
                for digit, (axis, bit) in zip(digits[1:], orders[target["dp"] & 1]):
                    if digit == 0:
                        target[axis] ^= bit
                block = target["dp"] * ctx_size + target["ctx"]
                table[dp * ctx_size + ctx, place * width:(place + 1) * width] = (
                    block * width + np.arange(width)
                )
    return table


def stage_pairs(stage, dp_size, ctx_size):
    pairs = []
    orders = stage_orders(dp_size, ctx_size)
    for dp in range(dp_size):
        for ctx in range(ctx_size):
            place = {"dp": dp, "ctx": ctx}
            axis, bit = ("dp", 1) if stage == 0 else orders[dp & 1][stage - 1]
            place[axis] ^= bit
            pairs.append((dp * ctx_size + ctx, place["dp"] * ctx_size + place["ctx"]))
    return pairs


def dot(a, b):
    return jnp.dot(a, b, preferred_element_type=jnp.float32)


def dot_nt(a, b):
    return lax.dot_general(a, b, NT, preferred_element_type=jnp.float32)


def load_body(place_ref, pos_ref, order_ref, latent_ref, rope_ref, query_ref, grad_ref, out_ref,
              lse_ref, wuk_ref, wuv_ref, latent_out, rope_out, query_out, grad_out, lse_out,
              delta_out, wuk_out, wuv_out, keys_out, values_out, flat_out, bias_out,
              pos, order, attn, sems, *, ctx_size):
    pairs = [(latent_ref, latent_out), (order_ref, order), (pos_ref, pos), (rope_ref, rope_out),
             (wuk_ref, wuk_out), (wuv_ref, wuv_out), (grad_ref, grad_out), (out_ref, attn),
             (lse_ref, lse_out), (query_ref, query_out)]
    copies = [pltpu.make_async_copy(a, b, sems.at[k]) for k, (a, b) in enumerate(pairs)]
    for copy in copies:
        copy.start()
    rows, _ = latent_out.shape
    for copy in copies[:3]:
        copy.wait()
    mine = place_ref[1]
    own_pos = jnp.broadcast_to(pos[mine], (rows, rows))
    for chunk in range(ctx_size):
        key_pos = pos[lax.rem(mine + chunk, ctx_size)]
        key_col = jnp.broadcast_to(key_pos, (rows, rows)).T
        bias_out[chunk * rows:(chunk + 1) * rows, :] = jnp.where(key_col <= own_pos, 0.0, MASKED)
    latent = latent_out[...]
    flat_out[...] = rows_first(latent, order[place_ref[0]])
    copies[4].wait()
    keys_out[...] = dot(latent, wuk_out[...]).astype(jnp.bfloat16)
    copies[5].wait()
    values_out[...] = dot(latent, wuv_out[...]).astype(jnp.bfloat16)
    copies[6].wait()
    copies[7].wait()
    for head in range(delta_out.shape[0]):
        cols = slice(head * DV, (head + 1) * DV)
        product = grad_out[:, cols].astype(jnp.float32) * attn[:, cols].astype(jnp.float32)
        delta_out[head:head + 1, :] = jnp.sum(product.T, axis=0, keepdims=True)
    for k in (3, 8, 9):
        copies[k].wait()


def rows_first(latent, order):
    width = latent.shape[1]
    spot = lax.broadcasted_iota(jnp.int32, (width, width), 0)
    pick = jnp.where(spot == order, 1.0, 0.0).astype(jnp.bfloat16)
    return dot(latent, pick).astype(jnp.bfloat16).T


def grads_body(place_ref, order_ref, *rest, ctx_size, start, count, first_col, group, has_prior,
               aliased, final, pieces):
    far_latents = rest[:ctx_size - 1]
    far_ropes = rest[ctx_size - 1:2 * ctx_size - 2]
    (latent_ref, rope_ref, query_ref, grad_ref, lse_ref, delta_ref, wuk_ref, wuv_ref, keys_ref,
     values_ref, flat_ref, bias_ref, *rest) = rest[2 * ctx_size - 2:]
    if has_prior:
        prior_ref, *rest = rest
    dq_ref, *rest = rest[aliased:]
    piece_refs, total_refs = rest[:pieces], rest[pieces:]
    rows, width = latent_ref.shape
    scale = 1.0 / math.sqrt(DQ)
    rope = jnp.concatenate([ref[...] for ref in (rope_ref, *far_ropes)], axis=1).T
    far = jnp.concatenate([ref[...] for ref in far_latents], axis=0)
    bias = bias_ref[...]
    flat = jnp.concatenate([flat_ref[...], rows_first(far, order_ref[place_ref[0]])], axis=1)
    rope_total = prior_ref[:, width:] if has_prior else 0.0
    latent_total = prior_ref[:, :width] if has_prior else 0.0
    for first in range(0, count, group):
        span = slice((start + first) * DN, (start + first + group) * DN)
        out_span = slice(first_col + first * DN, first_col + (first + group) * DN)
        wuk = wuk_ref[:, span]
        wuv = wuv_ref[:, span]
        keys_all = jnp.concatenate([keys_ref[:, span], dot(far, wuk).astype(jnp.bfloat16)], axis=0)
        values_all = jnp.concatenate(
            [values_ref[:, span], dot(far, wuv).astype(jnp.bfloat16)], axis=0
        )
        key_grads = []
        value_grads = []
        for inner in range(group):
            head = start + first + inner
            cols = slice(head * DN, (head + 1) * DN)
            wide = slice(head * DQ, (head + 1) * DQ)
            part = slice(inner * DN, (inner + 1) * DN)
            keys = jnp.concatenate([keys_all[:, part], rope], axis=1)
            query = query_ref[:, wide]
            grad = grad_ref[:, cols]
            delta = delta_ref[head:head + 1, :]
            lse = lse_ref[head:head + 1, :]
            weights = jnp.exp(dot_nt(keys, query) * scale - lse + bias)
            dots = dot_nt(values_all[:, part], grad)
            score_grad = (weights * (dots - delta) * scale).astype(jnp.bfloat16)
            dq_ref[:, wide] = dot(score_grad.T, keys).astype(jnp.bfloat16)
            key_grad = dot(score_grad, query)
            value_grads.append(dot(weights.astype(jnp.bfloat16), grad).astype(jnp.bfloat16))
            key_grads.append(key_grad[:, :DN].astype(jnp.bfloat16))
            rope_total = rope_total + key_grad[:, DN:]
        key_flat = jnp.concatenate(key_grads, axis=1)
        value_flat = jnp.concatenate(value_grads, axis=1)
        row = 0
        for piece_ref in piece_refs:
            size = piece_ref.shape[1]
            piece_ref[0, :, out_span] = dot(flat[row:row + size], key_flat).astype(jnp.bfloat16)
            piece_ref[1, :, out_span] = dot(flat[row:row + size], value_flat).astype(jnp.bfloat16)
            row += size
        latent_total = latent_total + dot_nt(key_flat, wuk) + dot_nt(value_flat, wuv)
    for chunk, total_ref in enumerate(total_refs):
        part = slice(chunk * rows, chunk * rows + total_ref.shape[0])
        total_ref[:, :width] = latent_total[part].astype(total_ref.dtype)
        total_ref[:, width:] = rope_total[part].astype(total_ref.dtype)


def in_vmem(array):
    return pltpu.with_memory_space_constraint(array, pltpu.VMEM)


def load(place, positions, order, latent, rope, query, grad_out, attn_out, lse, w_uk, w_uv):
    ctx_size = positions.shape[0]
    rows, width = latent.shape
    flat_size = w_uk.shape[1]
    like = lambda a: pltpu.VMEM(a.shape, a.dtype)
    vmem = pl.BlockSpec(memory_space=pltpu.VMEM)
    operands = [positions, order, latent, rope, query, grad_out, attn_out, lse, w_uk, w_uv]
    operands = [pltpu.with_memory_space_constraint(a, pltpu.HBM) for a in operands]
    outs = [like(a) for a in (latent, rope, query, grad_out, lse, lse, w_uk, w_uv)]
    outs += [pltpu.VMEM((rows, flat_size), jnp.bfloat16)] * 2
    outs += [pltpu.VMEM((width, rows), jnp.bfloat16), pltpu.VMEM((ctx_size * rows, rows), jnp.float32)]
    return pl.pallas_call(
        functools.partial(load_body, ctx_size=ctx_size),
        in_specs=[pl.BlockSpec(memory_space=pltpu.SMEM)]
        + [pl.BlockSpec(memory_space=pltpu.HBM)] * len(operands),
        out_specs=[vmem] * len(outs),
        out_shape=outs,
        scratch_shapes=[like(positions), like(order), like(attn_out), pltpu.SemaphoreType.DMA((10,))],
        compiler_params=pltpu.CompilerParams(vmem_limit_bytes=LOAD_LIMIT),
        name="load",
    )(place, *operands)


def chunk_grads(place, order, latents, ropes, loaded, prior, query_grad, pieces, *, start, count,
                chunk_heads, first_head, final):
    ctx_size = len(latents) + 1
    rows, width = loaded[0].shape
    blocks = order.shape[0]
    smem = pl.BlockSpec(memory_space=pltpu.SMEM)
    vmem = pl.BlockSpec(memory_space=pltpu.VMEM)
    buffers = ([] if query_grad is None else [query_grad]) + list(pieces)
    operands = [*latents, *ropes, *loaded] + ([] if prior is None else [prior]) + buffers
    operands = [in_vmem(a) for a in operands]
    sizes = [width >> (s + 1) for s in range(blocks.bit_length() - 1)]
    sizes.append(sizes[-1])
    if final:
        totals = [pltpu.VMEM((rows, width + DR), jnp.bfloat16)] * ctx_size
    else:
        totals = [pltpu.VMEM((ctx_size * rows, width + DR), jnp.float32)]
    first_buffer = 2 + len(operands) - len(buffers)
    outs = pl.pallas_call(
        functools.partial(grads_body, ctx_size=ctx_size, start=start, count=count,
                          first_col=(start - first_head) * DN, group=math.gcd(count, GROUP),
                          has_prior=prior is not None, aliased=len(buffers), final=final,
                          pieces=len(sizes)),
        in_specs=[smem] + [vmem] * (1 + len(operands)),
        out_specs=[vmem] * (1 + len(sizes) + len(totals)),
        out_shape=[pltpu.VMEM(loaded[2].shape, jnp.bfloat16)]
        + [pltpu.VMEM((2, size, chunk_heads * DN), jnp.bfloat16) for size in sizes] + totals,
        input_output_aliases={first_buffer + k: k for k in range(len(buffers))},
        compiler_params=pltpu.CompilerParams(vmem_limit_bytes=VMEM_LIMIT),
        name="grads",
    )(place, order, *operands)
    return outs[0], outs[1:1 + len(sizes)], outs[1 + len(sizes):]


def piece_sum(refs, offsets, size):
    total = refs[0][...].astype(jnp.float32)
    for ref, first in zip(refs[1:], offsets):
        total = total + ref[:, first:first + size, :].astype(jnp.float32)
    return total.astype(jnp.bfloat16)


def add_body(*refs, offsets):
    refs[-1][...] = piece_sum(refs[:-1], offsets, refs[0].shape[1])


def last_body(*refs):
    *refs, uk_ref, uv_ref = refs
    width = refs[0].shape[2]
    for chunk in range(len(refs) // 2):
        keep_ref, arrival_ref = refs[2 * chunk:2 * chunk + 2]
        total = piece_sum((keep_ref, arrival_ref), (0,), keep_ref.shape[1])
        uk_ref[:, chunk * width:(chunk + 1) * width] = total[0]
        uv_ref[:, chunk * width:(chunk + 1) * width] = total[1]


def piece_offsets(pieces, stage):
    sizes = [p.shape[1] for p in pieces]
    return tuple(sum(sizes[past + 1:stage]) for past in range(stage))


def add_arrivals(pieces, stage, arrivals):
    operands = [in_vmem(a) for a in (pieces[stage], *arrivals)]
    vmem = pl.BlockSpec(memory_space=pltpu.VMEM)
    return pl.pallas_call(
        functools.partial(add_body, offsets=piece_offsets(pieces, stage)),
        in_specs=[vmem] * len(operands),
        out_specs=vmem,
        out_shape=pltpu.VMEM(pieces[stage].shape, jnp.bfloat16),
        compiler_params=pltpu.CompilerParams(vmem_limit_bytes=ADD_LIMIT),
        name="add",
    )(*operands)


def last_sums(keeps, arrivals):
    operands = [in_vmem(a) for pair in zip(keeps, arrivals) for a in pair]
    _, size, width = keeps[0].shape
    vmem = pl.BlockSpec(memory_space=pltpu.VMEM)
    out = jax.ShapeDtypeStruct((size, width * len(keeps)), jnp.bfloat16)
    return pl.pallas_call(
        last_body,
        in_specs=[vmem] * len(operands),
        out_specs=[vmem] * 2,
        out_shape=[out, out],
        compiler_params=pltpu.CompilerParams(vmem_limit_bytes=ADD_LIMIT),
        name="last",
    )(*operands)


def kernel_plan(head_count):
    groups = head_count // math.gcd(head_count, GROUP)
    if groups % 4:
        return [(0, head_count, 0)]
    half = head_count // 2
    return [(0, half, 0), (half, half // 2, 1), (half + half // 2, half // 2, 1)]


def shifted(value, axis, steps):
    count = lax.axis_size(axis)
    return lax.ppermute(value, axis, [(s, (s + steps) % count) for s in range(count)])


def on_device(latent, rope, query, grad_out, attn_out, lse, positions, w_uk, w_uv):
    dp_size, ctx_size, head_size = (lax.axis_size(a) for a in ("dp", "ctx", "head"))
    rows, width = latent.shape[1:]
    my_ctx = lax.axis_index("ctx")
    my_place = lax.axis_index("dp") * ctx_size + my_ctx
    place = jnp.stack([my_place, my_ctx]).astype(jnp.int32)
    order = jnp.asarray(row_table(dp_size, ctx_size, width))[:, None, :]
    rope_cols = rope[0].T
    latents = [shifted(latent[0], "ctx", -s) for s in range(1, ctx_size)]
    ropes = [shifted(rope_cols, "ctx", -s) for s in range(1, ctx_size)]
    loaded = load(place, positions.reshape(ctx_size, 1, rows), order, latent[0], rope_cols, query[0],
                  grad_out[0], attn_out[0], lse[0], w_uk, w_uv)
    plan = kernel_plan(lse.shape[1])
    chunks = plan[-1][2] + 1
    chunk_heads = lse.shape[1] // chunks
    prior = query_grad = None
    chunk_pieces = [()] * chunks
    for number, (start, count, chunk) in enumerate(plan):
        query_grad, pieces, totals = chunk_grads(
            place, order, latents, ropes, loaded, prior, query_grad, chunk_pieces[chunk],
            start=start, count=count, chunk_heads=chunk_heads, first_head=chunk * chunk_heads,
            final=number + 1 == len(plan),
        )
        prior = totals[0]
        chunk_pieces[chunk] = pieces
    summed = totals[0].astype(jnp.float32)
    for s in range(1, ctx_size):
        summed = summed + shifted(totals[s], "ctx", s).astype(jnp.float32)
    for bit in bits_of(head_size):
        mine = summed.astype(jnp.bfloat16)
        other = lax.ppermute(mine, "head", [(s, s ^ bit) for s in range(head_size)])
        summed = mine.astype(jnp.float32) + other.astype(jnp.float32)
    keeps = []
    lasts = []
    for pieces in chunk_pieces:
        arrivals = []
        for stage in range(len(pieces) - 1):
            value = add_arrivals(pieces, stage, arrivals) if stage else pieces[0]
            pairs = stage_pairs(stage, dp_size, ctx_size)
            arrivals.append(lax.ppermute(value, ("dp", "ctx"), pairs))
        keeps.append(add_arrivals(pieces, len(pieces) - 1, arrivals[:-1]))
        lasts.append(arrivals[-1])
    weight_uk, weight_uv = last_sums(keeps, lasts)
    return (
        query_grad[None],
        summed[None, :, :width],
        summed[None, :, width:],
        weight_uk,
        weight_uv,
    )


def solution(mesh):
    return jax.shard_map(
        on_device,
        mesh=mesh,
        in_specs=(
            P("dp", "ctx", None),
            P("dp", "ctx", None),
            P("dp", "ctx", "head"),
            P("dp", "ctx", "head"),
            P("dp", "ctx", "head"),
            P("dp", "head", "ctx"),
            P("dp", None),
            P(None, "head"),
            P(None, "head"),
        ),
        out_specs=(
            P("dp", "ctx", "head"),
            P("dp", "ctx", None),
            P("dp", "ctx", None),
            P(("dp", "ctx"), "head"),
            P(("dp", "ctx"), "head"),
        ),
        check_vma=False,
    )
```

```python
import functools
import math

import jax
import jax.numpy as jnp
import numpy as np
from jax import lax
from jax.experimental import pallas as pl
from jax.experimental.pallas import tpu as pltpu
from jax.sharding import PartitionSpec as P


DR = 64
DN = 128
DV = 128
DQ = DN + DR

MASKED = -1e30
GROUP = 4
VMEM_LIMIT = 6 << 20
LOAD_LIMIT = 4 << 20
ADD_LIMIT = 2 << 20
NT = (((1,), (1,)), ((), ()))


def bits_of(count):
    return [1 << b for b in range(count.bit_length() - 1)]


def stage_orders(dp_size, ctx_size):
    outer = [("dp", bit) for bit in bits_of(dp_size)[1:]]
    inner = [("ctx", bit) for bit in bits_of(ctx_size)]
    return outer + inner, inner + outer


def row_table(dp_size, ctx_size, rows):
    orders = stage_orders(dp_size, ctx_size)
    blocks = dp_size * ctx_size
    width = rows // blocks
    table = np.zeros((blocks, rows), np.int32)
    for dp in range(dp_size):
        for ctx in range(ctx_size):
            for place in range(blocks):
                digits = [(place >> b) & 1 for b in reversed(range(blocks.bit_length() - 1))]
                target = {"dp": dp, "ctx": ctx}
                if digits[0] == 0:
                    target["dp"] ^= 1
                for digit, (axis, bit) in zip(digits[1:], orders[target["dp"] & 1]):
                    if digit == 0:
                        target[axis] ^= bit
                block = target["dp"] * ctx_size + target["ctx"]
                table[dp * ctx_size + ctx, place * width:(place + 1) * width] = (
                    block * width + np.arange(width)
                )
    return table


def stage_pairs(stage, dp_size, ctx_size):
    pairs = []
    orders = stage_orders(dp_size, ctx_size)
    for dp in range(dp_size):
        for ctx in range(ctx_size):
            place = {"dp": dp, "ctx": ctx}
            axis, bit = ("dp", 1) if stage == 0 else orders[dp & 1][stage - 1]
            place[axis] ^= bit
            pairs.append((dp * ctx_size + ctx, place["dp"] * ctx_size + place["ctx"]))
    return pairs


def dot(a, b):
    return jnp.dot(a, b, preferred_element_type=jnp.float32)


def dot_nt(a, b):
    return lax.dot_general(a, b, NT, preferred_element_type=jnp.float32)


def load_body(place_ref, pos_ref, order_ref, latent_ref, rope_ref, query_ref, grad_ref, out_ref,
              lse_ref, wuk_ref, wuv_ref, latent_out, rope_out, query_out, grad_out, lse_out,
              delta_out, wuk_out, wuv_out, keys_out, values_out, flat_out, bias_out,
              pos, order, attn, sems, *, ctx_size):
    pairs = [(latent_ref, latent_out), (order_ref, order), (pos_ref, pos), (rope_ref, rope_out),
             (wuk_ref, wuk_out), (wuv_ref, wuv_out), (grad_ref, grad_out), (out_ref, attn),
             (lse_ref, lse_out), (query_ref, query_out)]
    copies = [pltpu.make_async_copy(a, b, sems.at[k]) for k, (a, b) in enumerate(pairs)]
    for copy in copies:
        copy.start()
    rows, _ = latent_out.shape
    for copy in copies[:3]:
        copy.wait()
    mine = place_ref[1]
    own_pos = jnp.broadcast_to(pos[mine], (rows, rows))
    for chunk in range(ctx_size):
        key_pos = pos[lax.rem(mine + chunk, ctx_size)]
        key_col = jnp.broadcast_to(key_pos, (rows, rows)).T
        bias_out[chunk * rows:(chunk + 1) * rows, :] = jnp.where(key_col <= own_pos, 0.0, MASKED)
    latent = latent_out[...]
    flat_out[...] = rows_first(latent, order[place_ref[0]])
    copies[4].wait()
    keys_out[...] = dot(latent, wuk_out[...]).astype(jnp.bfloat16)
    copies[5].wait()
    values_out[...] = dot(latent, wuv_out[...]).astype(jnp.bfloat16)
    copies[6].wait()
    copies[7].wait()
    for head in range(delta_out.shape[0]):
        cols = slice(head * DV, (head + 1) * DV)
        product = grad_out[:, cols].astype(jnp.float32) * attn[:, cols].astype(jnp.float32)
        delta_out[head:head + 1, :] = jnp.sum(product.T, axis=0, keepdims=True)
    for k in (3, 8, 9):
        copies[k].wait()


def rows_first(latent, order):
    width = latent.shape[1]
    spot = lax.broadcasted_iota(jnp.int32, (width, width), 0)
    pick = jnp.where(spot == order, 1.0, 0.0).astype(jnp.bfloat16)
    return dot(latent, pick).astype(jnp.bfloat16).T


def grads_body(place_ref, order_ref, *rest, ctx_size, group):
    far_latents = rest[:ctx_size - 1]
    far_ropes = rest[ctx_size - 1:2 * ctx_size - 2]
    (latent_ref, rope_ref, query_ref, grad_ref, lse_ref, delta_ref, wuk_ref, wuv_ref, keys_ref,
     values_ref, flat_ref, bias_ref, *rest) = rest[2 * ctx_size - 2:]
    dq_ref, key_out, value_out, flat_out, *total_refs = rest
    rows, _ = latent_ref.shape
    scale = 1.0 / math.sqrt(DQ)
    rope = jnp.concatenate([ref[...] for ref in (rope_ref, *far_ropes)], axis=1).T
    far = jnp.concatenate([ref[...] for ref in far_latents], axis=0)
    bias = bias_ref[...]
    flat_out[...] = jnp.concatenate(
        [flat_ref[...], rows_first(far, order_ref[place_ref[0]])], axis=1
    )
    rope_total = 0.0
    latent_total = 0.0
    for first in range(0, lse_ref.shape[0], group):
        span = slice(first * DN, (first + group) * DN)
        wuk = wuk_ref[:, span]
        wuv = wuv_ref[:, span]
        keys_all = jnp.concatenate([keys_ref[:, span], dot(far, wuk).astype(jnp.bfloat16)], axis=0)
        values_all = jnp.concatenate(
            [values_ref[:, span], dot(far, wuv).astype(jnp.bfloat16)], axis=0
        )
        key_grads = []
        value_grads = []
        for inner in range(group):
            head = first + inner
            cols = slice(head * DN, (head + 1) * DN)
            wide = slice(head * DQ, (head + 1) * DQ)
            part = slice(inner * DN, (inner + 1) * DN)
            keys = jnp.concatenate([keys_all[:, part], rope], axis=1)
            query = query_ref[:, wide]
            grad = grad_ref[:, cols]
            delta = delta_ref[head:head + 1, :]
            lse = lse_ref[head:head + 1, :]
            weights = jnp.exp(dot_nt(keys, query) * scale - lse + bias)
            dots = dot_nt(values_all[:, part], grad)
            score_grad = (weights * (dots - delta) * scale).astype(jnp.bfloat16)
            dq_ref[:, wide] = dot(score_grad.T, keys).astype(jnp.bfloat16)
            key_grad = dot(score_grad, query)
            value_grads.append(dot(weights.astype(jnp.bfloat16), grad).astype(jnp.bfloat16))
            key_grads.append(key_grad[:, :DN].astype(jnp.bfloat16))
            rope_total = rope_total + key_grad[:, DN:]
        key_flat = jnp.concatenate(key_grads, axis=1)
        value_flat = jnp.concatenate(value_grads, axis=1)
        key_out[:, span] = key_flat
        value_out[:, span] = value_flat
        latent_total = latent_total + dot_nt(key_flat, wuk) + dot_nt(value_flat, wuv)
    for chunk, total_ref in enumerate(total_refs):
        part = slice(chunk * rows, (chunk + 1) * rows)
        total_ref[:rows, :] = latent_total[part].astype(jnp.bfloat16)
        rope_cols = rope_total[part].T.astype(jnp.bfloat16)
        extra = total_ref.shape[0] - rows
        for k in range(DR // extra):
            total_ref[rows:, k * rows:(k + 1) * rows] = rope_cols[k * extra:(k + 1) * extra]


def write_pieces(piece_refs, span, flat, key_flat, value_flat):
    row = 0
    for piece_ref in piece_refs:
        size = piece_ref.shape[1]
        piece_ref[0, :, span] = dot(flat[row:row + size], key_flat).astype(jnp.bfloat16)
        piece_ref[1, :, span] = dot(flat[row:row + size], value_flat).astype(jnp.bfloat16)
        row += size


def weights_body(flat_ref, key_ref, value_ref, *piece_refs, start):
    flat = flat_ref[...]
    count = piece_refs[0].shape[2]
    step = math.gcd(count, 256)
    for first in range(0, count, step):
        part = slice(start + first, start + first + step)
        span = slice(first, first + step)
        write_pieces(piece_refs, span, flat, key_ref[:, part], value_ref[:, part])


def store_body(source_ref, out_ref, sem):
    copy = pltpu.make_async_copy(source_ref, out_ref, sem)
    copy.start()
    copy.wait()


def store(array):
    return pl.pallas_call(
        store_body,
        in_specs=[pl.BlockSpec(memory_space=pltpu.VMEM)],
        out_specs=pl.BlockSpec(memory_space=pltpu.HBM),
        out_shape=pltpu.HBM(array.shape, array.dtype),
        scratch_shapes=[pltpu.SemaphoreType.DMA(())],
        compiler_params=pltpu.CompilerParams(vmem_limit_bytes=ADD_LIMIT),
        name="store",
    )(in_vmem(array))


def piece_sizes(width, blocks):
    sizes = [width >> (s + 1) for s in range(blocks.bit_length() - 1)]
    return sizes + sizes[-1:]


def piece_shapes(width, blocks, columns):
    return [pltpu.VMEM((2, size, columns), jnp.bfloat16) for size in piece_sizes(width, blocks)]


def chunk_weights(flat, key_flat, value_flat, blocks, start, count):
    vmem = pl.BlockSpec(memory_space=pltpu.VMEM)
    shapes = piece_shapes(flat.shape[0], blocks, count * DN)
    return pl.pallas_call(
        functools.partial(weights_body, start=start * DN),
        in_specs=[vmem] * 3,
        out_specs=[vmem] * len(shapes),
        out_shape=shapes,
        compiler_params=pltpu.CompilerParams(vmem_limit_bytes=VMEM_LIMIT),
        name="weights",
    )(*[in_vmem(a) for a in (flat, key_flat, value_flat)])


def in_vmem(array):
    return pltpu.with_memory_space_constraint(array, pltpu.VMEM)


def load(place, positions, order, latent, rope, query, grad_out, attn_out, lse, w_uk, w_uv):
    ctx_size = positions.shape[0]
    rows, width = latent.shape
    flat_size = w_uk.shape[1]
    like = lambda a: pltpu.VMEM(a.shape, a.dtype)
    vmem = pl.BlockSpec(memory_space=pltpu.VMEM)
    operands = [positions, order, latent, rope, query, grad_out, attn_out, lse, w_uk, w_uv]
    operands = [pltpu.with_memory_space_constraint(a, pltpu.HBM) for a in operands]
    outs = [like(a) for a in (latent, rope, query, grad_out, lse, lse, w_uk, w_uv)]
    outs += [pltpu.VMEM((rows, flat_size), jnp.bfloat16)] * 2
    outs += [pltpu.VMEM((width, rows), jnp.bfloat16), pltpu.VMEM((ctx_size * rows, rows), jnp.float32)]
    return pl.pallas_call(
        functools.partial(load_body, ctx_size=ctx_size),
        in_specs=[pl.BlockSpec(memory_space=pltpu.SMEM)]
        + [pl.BlockSpec(memory_space=pltpu.HBM)] * len(operands),
        out_specs=[vmem] * len(outs),
        out_shape=outs,
        scratch_shapes=[like(positions), like(order), like(attn_out), pltpu.SemaphoreType.DMA((10,))],
        compiler_params=pltpu.CompilerParams(vmem_limit_bytes=LOAD_LIMIT),
        name="load",
    )(place, *operands)


def all_grads(place, order, latents, ropes, loaded):
    ctx_size = len(latents) + 1
    rows, width = loaded[0].shape
    head_count = loaded[4].shape[0]
    spread = pltpu.VMEM((ctx_size * rows, head_count * DN), jnp.bfloat16)
    total = pltpu.VMEM((rows + DR * rows // width, width), jnp.bfloat16)
    flat = pltpu.VMEM((width, ctx_size * rows), jnp.bfloat16)
    operands = [in_vmem(a) for a in (order, *latents, *ropes, *loaded)]
    vmem = pl.BlockSpec(memory_space=pltpu.VMEM)
    outs = pl.pallas_call(
        functools.partial(grads_body, ctx_size=ctx_size, group=math.gcd(head_count, GROUP)),
        in_specs=[pl.BlockSpec(memory_space=pltpu.SMEM)] + [vmem] * len(operands),
        out_specs=[vmem] * (4 + ctx_size),
        out_shape=[pltpu.VMEM(loaded[2].shape, jnp.bfloat16), spread, spread, flat]
        + [total] * ctx_size,
        compiler_params=pltpu.CompilerParams(vmem_limit_bytes=VMEM_LIMIT),
        name="grads",
    )(place, *operands)
    return outs[0], outs[1], outs[2], outs[3], outs[4:]


def piece_sum(refs, offsets, size):
    total = refs[0][...].astype(jnp.float32)
    for ref, first in zip(refs[1:], offsets):
        total = total + ref[:, first:first + size, :].astype(jnp.float32)
    return total.astype(jnp.bfloat16)


def add_body(*refs, offsets):
    refs[-1][...] = piece_sum(refs[:-1], offsets, refs[0].shape[1])


def finish_body(mine_ref, other_ref, latent_out, rope_out):
    rows = latent_out.shape[0]
    total = mine_ref[...].astype(jnp.float32) + other_ref[...].astype(jnp.float32)
    latent_out[...] = total[:rows]
    extra = total.shape[0] - rows
    for k in range(rope_out.shape[0] // extra):
        rope_out[k * extra:(k + 1) * extra, :] = total[rows:, k * rows:(k + 1) * rows]


def finish(mine, other, rows):
    width = mine.shape[1]
    vmem = pl.BlockSpec(memory_space=pltpu.VMEM)
    return pl.pallas_call(
        finish_body,
        in_specs=[vmem] * 2,
        out_specs=[vmem] * 2,
        out_shape=[jax.ShapeDtypeStruct((rows, width), jnp.float32),
                   jax.ShapeDtypeStruct((DR, rows), jnp.float32)],
        compiler_params=pltpu.CompilerParams(vmem_limit_bytes=ADD_LIMIT),
        name="finish",
    )(in_vmem(mine), in_vmem(other))


def last_body(*refs):
    *refs, uk_ref, uv_ref = refs
    first = 0
    for keep_ref, arrival_ref in zip(refs[::2], refs[1::2]):
        total = piece_sum((keep_ref, arrival_ref), (0,), keep_ref.shape[1])
        width = keep_ref.shape[2]
        uk_ref[:, first:first + width] = total[0]
        uv_ref[:, first:first + width] = total[1]
        first += width


def piece_offsets(pieces, stage):
    sizes = [p.shape[1] for p in pieces]
    return tuple(sum(sizes[past + 1:stage]) for past in range(stage))


def add_arrivals(pieces, stage, arrivals):
    operands = [in_vmem(a) for a in (pieces[stage], *arrivals)]
    vmem = pl.BlockSpec(memory_space=pltpu.VMEM)
    return pl.pallas_call(
        functools.partial(add_body, offsets=piece_offsets(pieces, stage)),
        in_specs=[vmem] * len(operands),
        out_specs=vmem,
        out_shape=pltpu.VMEM(pieces[stage].shape, jnp.bfloat16),
        compiler_params=pltpu.CompilerParams(vmem_limit_bytes=ADD_LIMIT),
        name="add",
    )(*operands)


def last_sums(keeps, arrivals):
    operands = [in_vmem(a) for pair in zip(keeps, arrivals) for a in pair]
    size = keeps[0].shape[1]
    vmem = pl.BlockSpec(memory_space=pltpu.VMEM)
    out = jax.ShapeDtypeStruct((size, sum(k.shape[2] for k in keeps)), jnp.bfloat16)
    return pl.pallas_call(
        last_body,
        in_specs=[vmem] * len(operands),
        out_specs=[vmem] * 2,
        out_shape=[out, out],
        compiler_params=pltpu.CompilerParams(vmem_limit_bytes=ADD_LIMIT),
        name="last",
    )(*operands)


def shifted(value, axis, steps):
    count = lax.axis_size(axis)
    return lax.ppermute(value, axis, [(s, (s + steps) % count) for s in range(count)])


def on_device(latent, rope, query, grad_out, attn_out, lse, positions, w_uk, w_uv):
    dp_size, ctx_size, head_size = (lax.axis_size(a) for a in ("dp", "ctx", "head"))
    rows, width = latent.shape[1:]
    my_ctx = lax.axis_index("ctx")
    my_place = lax.axis_index("dp") * ctx_size + my_ctx
    place = jnp.stack([my_place, my_ctx]).astype(jnp.int32)
    order = jnp.asarray(row_table(dp_size, ctx_size, width))[:, None, :]
    rope_cols = rope[0].T
    latents = [shifted(latent[0], "ctx", -s) for s in range(1, ctx_size)]
    ropes = [shifted(rope_cols, "ctx", -s) for s in range(1, ctx_size)]
    loaded = load(place, positions.reshape(ctx_size, 1, rows), order, latent[0], rope_cols, query[0],
                  grad_out[0], attn_out[0], lse[0], w_uk, w_uv)
    query_grad, key_flat, value_flat, flat, totals = all_grads(place, order, latents, ropes, loaded)
    head_count = lse.shape[1]
    quarter = head_count // 4
    last = quarter // 2
    counts = [quarter, head_count - quarter - last, last] if quarter >= GROUP else [head_count]
    chunk_pieces = []
    for chunk, count in enumerate(counts):
        chunk_pieces.append(chunk_weights(flat, key_flat, value_flat, dp_size * ctx_size,
                                          sum(counts[:chunk]), count))
    query_grad = store(query_grad)
    summed = totals[0].astype(jnp.float32)
    for s in range(1, ctx_size):
        summed = summed + shifted(totals[s], "ctx", s).astype(jnp.float32)
    mine, other = summed.astype(jnp.bfloat16), jnp.zeros(summed.shape, jnp.bfloat16)
    for bit in bits_of(head_size):
        mine = summed.astype(jnp.bfloat16)
        other = lax.ppermute(mine, "head", [(s, s ^ bit) for s in range(head_size)])
        summed = mine.astype(jnp.float32) + other.astype(jnp.float32)
    grad_latent, grad_rope = finish(mine, other, rows)
    keeps = []
    lasts = []
    for pieces in chunk_pieces:
        arrivals = []
        for stage in range(len(pieces) - 1):
            value = add_arrivals(pieces, stage, arrivals) if stage else pieces[0]
            pairs = stage_pairs(stage, dp_size, ctx_size)
            arrivals.append(lax.ppermute(value, ("dp", "ctx"), pairs))
        keeps.append(add_arrivals(pieces, len(pieces) - 1, arrivals[:-1]))
        lasts.append(arrivals[-1])
    weight_uk, weight_uv = last_sums(keeps, lasts)
    return (
        query_grad[None],
        grad_latent[None],
        grad_rope.T[None],
        weight_uk,
        weight_uv,
    )


def solution(mesh):
    return jax.shard_map(
        on_device,
        mesh=mesh,
        in_specs=(
            P("dp", "ctx", None),
            P("dp", "ctx", None),
            P("dp", "ctx", "head"),
            P("dp", "ctx", "head"),
            P("dp", "ctx", "head"),
            P("dp", "head", "ctx"),
            P("dp", None),
            P(None, "head"),
            P(None, "head"),
        ),
        out_specs=(
            P("dp", "ctx", "head"),
            P("dp", "ctx", None),
            P("dp", "ctx", None),
            P(("dp", "ctx"), "head"),
            P(("dp", "ctx"), "head"),
        ),
        check_vma=False,
    )
```

```python
import functools
import math

import jax
import jax.numpy as jnp
import numpy as np
from jax import lax
from jax.experimental import pallas as pl
from jax.experimental.pallas import tpu as pltpu
from jax.sharding import PartitionSpec as P


DR = 64
DN = 128
DV = 128
DQ = DN + DR

MASKED = -1e30
GROUP = 8
VMEM_LIMIT = 6 << 20
LIMIT_A_TOKEN = 24 << 10
LOAD_LIMIT = 4 << 20
ADD_LIMIT = 2 << 20
NT = (((1,), (1,)), ((), ()))


def bits_of(count):
    return [1 << b for b in range(count.bit_length() - 1)]


def stage_orders(dp_size, ctx_size):
    outer = [("dp", bit) for bit in bits_of(dp_size)[1:]]
    inner = [("ctx", bit) for bit in bits_of(ctx_size)]
    return outer + inner, inner + outer


def row_table(dp_size, ctx_size, rows):
    orders = stage_orders(dp_size, ctx_size)
    blocks = dp_size * ctx_size
    width = rows // blocks
    table = np.zeros((blocks, rows), np.int32)
    for dp in range(dp_size):
        for ctx in range(ctx_size):
            for place in range(blocks):
                digits = [(place >> b) & 1 for b in reversed(range(blocks.bit_length() - 1))]
                target = {"dp": dp, "ctx": ctx}
                if digits[0] == 0:
                    target["dp"] ^= 1
                for digit, (axis, bit) in zip(digits[1:], orders[target["dp"] & 1]):
                    if digit == 0:
                        target[axis] ^= bit
                block = target["dp"] * ctx_size + target["ctx"]
                table[dp * ctx_size + ctx, place * width:(place + 1) * width] = (
                    block * width + np.arange(width)
                )
    return table


def stage_pairs(stage, dp_size, ctx_size):
    pairs = []
    orders = stage_orders(dp_size, ctx_size)
    for dp in range(dp_size):
        for ctx in range(ctx_size):
            place = {"dp": dp, "ctx": ctx}
            axis, bit = ("dp", 1) if stage == 0 else orders[dp & 1][stage - 1]
            place[axis] ^= bit
            pairs.append((dp * ctx_size + ctx, place["dp"] * ctx_size + place["ctx"]))
    return pairs


def dot(a, b):
    return jnp.dot(a, b, preferred_element_type=jnp.float32)


def dot_nt(a, b):
    return lax.dot_general(a, b, NT, preferred_element_type=jnp.float32)


def load_body(place_ref, pos_ref, order_ref, latent_ref, rope_ref, query_ref, grad_ref, out_ref,
              lse_ref, wuk_ref, wuv_ref, latent_out, rope_out, query_out, grad_out, lse_out,
              delta_out, wuk_out, wuv_out, keys_out, values_out, flat_out, bias_out,
              pos, order, attn, sems, *, ctx_size):
    pairs = [(latent_ref, latent_out), (order_ref, order), (pos_ref, pos), (rope_ref, rope_out),
             (wuk_ref, wuk_out), (wuv_ref, wuv_out), (grad_ref, grad_out), (out_ref, attn),
             (lse_ref, lse_out), (query_ref, query_out)]
    copies = [pltpu.make_async_copy(a, b, sems.at[k]) for k, (a, b) in enumerate(pairs)]
    for copy in copies:
        copy.start()
    rows, _ = latent_out.shape
    for copy in copies[:3]:
        copy.wait()
    mine = place_ref[1]
    own_pos = jnp.broadcast_to(pos[mine], (rows, rows))
    for chunk in range(ctx_size):
        key_pos = pos[lax.rem(mine + chunk, ctx_size)]
        key_col = jnp.broadcast_to(key_pos, (rows, rows)).T
        bias_out[chunk * rows:(chunk + 1) * rows, :] = jnp.where(key_col <= own_pos, 0.0, MASKED)
    latent = latent_out[...]
    flat_out[...] = rows_first(latent, order[place_ref[0]])
    copies[4].wait()
    keys_out[...] = dot(latent, wuk_out[...]).astype(jnp.bfloat16)
    copies[5].wait()
    values_out[...] = dot(latent, wuv_out[...]).astype(jnp.bfloat16)
    copies[6].wait()
    copies[7].wait()
    for head in range(delta_out.shape[0]):
        cols = slice(head * DV, (head + 1) * DV)
        product = grad_out[:, cols].astype(jnp.float32) * attn[:, cols].astype(jnp.float32)
        delta_out[head:head + 1, :] = jnp.sum(product.T, axis=0, keepdims=True)
    for k in (3, 8, 9):
        copies[k].wait()


def rows_first(latent, order):
    width = latent.shape[1]
    spot = lax.broadcasted_iota(jnp.int32, (width, width), 0)
    pick = jnp.where(spot == order, 1.0, 0.0).astype(jnp.bfloat16)
    return dot(latent, pick).astype(jnp.bfloat16).T


def grads_body(place_ref, order_ref, *rest, ctx_size, group):
    far_latents = rest[:ctx_size - 1]
    far_ropes = rest[ctx_size - 1:2 * ctx_size - 2]
    (latent_ref, rope_ref, query_ref, grad_ref, lse_ref, delta_ref, wuk_ref, wuv_ref, keys_ref,
     values_ref, flat_ref, bias_ref, *rest) = rest[2 * ctx_size - 2:]
    dq_ref, key_out, value_out, flat_out, *total_refs = rest
    rows, _ = latent_ref.shape
    scale = 1.0 / math.sqrt(DQ)
    rope = jnp.concatenate([ref[...] for ref in (rope_ref, *far_ropes)], axis=1).T
    far = jnp.concatenate([ref[...] for ref in far_latents], axis=0)
    bias = bias_ref[...]
    flat_out[...] = jnp.concatenate(
        [flat_ref[...], rows_first(far, order_ref[place_ref[0]])], axis=1
    )
    rope_total = 0.0
    latent_total = 0.0
    for first in range(0, lse_ref.shape[0], group):
        span = slice(first * DN, (first + group) * DN)
        wuk = wuk_ref[:, span]
        wuv = wuv_ref[:, span]
        keys_all = jnp.concatenate([keys_ref[:, span], dot(far, wuk).astype(jnp.bfloat16)], axis=0)
        values_all = jnp.concatenate(
            [values_ref[:, span], dot(far, wuv).astype(jnp.bfloat16)], axis=0
        )
        key_grads = []
        value_grads = []
        stages = []
        for inner in range(group + 2):
            if inner < group:
                head = first + inner
                cols = slice(head * DN, (head + 1) * DN)
                wide = slice(head * DQ, (head + 1) * DQ)
                part = slice(inner * DN, (inner + 1) * DN)
                keys = jnp.concatenate([keys_all[:, part], rope], axis=1)
                query = query_ref[:, wide]
                grad = grad_ref[:, cols]
                stages.append([head, wide, keys, query, grad, dot_nt(keys, query),
                               dot_nt(values_all[:, part], grad)])
            if 0 <= inner - 2:
                wide, keys, query, grad, score_grad, weights_b = stages[inner - 2]
                dq_ref[:, wide] = dot(score_grad.T, keys).astype(jnp.bfloat16)
                key_grad = dot(score_grad, query)
                value_grads.append(dot(weights_b, grad).astype(jnp.bfloat16))
                key_grads.append(key_grad[:, :DN].astype(jnp.bfloat16))
                rope_total = rope_total + key_grad[:, DN:]
            if 0 <= inner - 1 < group:
                head, wide, keys, query, grad, scores, dots = stages[inner - 1]
                weights = jnp.exp(scores * scale - lse_ref[head:head + 1, :] + bias)
                score_grad = weights * (dots - delta_ref[head:head + 1, :]) * scale
                stages[inner - 1] = (wide, keys, query, grad, score_grad.astype(jnp.bfloat16),
                                     weights.astype(jnp.bfloat16))
        key_flat = jnp.concatenate(key_grads, axis=1)
        value_flat = jnp.concatenate(value_grads, axis=1)
        key_out[:, span] = key_flat
        value_out[:, span] = value_flat
        latent_total = latent_total + dot_nt(key_flat, wuk) + dot_nt(value_flat, wuv)
    for chunk, total_ref in enumerate(total_refs):
        part = slice(chunk * rows, (chunk + 1) * rows)
        total_ref[:rows, :] = latent_total[part].astype(jnp.bfloat16)
        rope_cols = rope_total[part].T.astype(jnp.bfloat16)
        extra = total_ref.shape[0] - rows
        for k in range(DR // extra):
            total_ref[rows:, k * rows:(k + 1) * rows] = rope_cols[k * extra:(k + 1) * extra]


def write_pieces(piece_refs, span, flat, key_flat, value_flat):
    row = 0
    for piece_ref in piece_refs:
        size = piece_ref.shape[1]
        piece_ref[0, :, span] = dot(flat[row:row + size], key_flat).astype(jnp.bfloat16)
        piece_ref[1, :, span] = dot(flat[row:row + size], value_flat).astype(jnp.bfloat16)
        row += size


def weights_body(flat_ref, key_ref, value_ref, *piece_refs, start):
    flat = flat_ref[...]
    count = piece_refs[0].shape[2]
    step = math.gcd(count, 256)
    for first in range(0, count, step):
        part = slice(start + first, start + first + step)
        span = slice(first, first + step)
        write_pieces(piece_refs, span, flat, key_ref[:, part], value_ref[:, part])


def store_body(source_ref, out_ref, sem):
    copy = pltpu.make_async_copy(source_ref, out_ref, sem)
    copy.start()
    copy.wait()


def store(array):
    return pl.pallas_call(
        store_body,
        in_specs=[pl.BlockSpec(memory_space=pltpu.VMEM)],
        out_specs=pl.BlockSpec(memory_space=pltpu.HBM),
        out_shape=pltpu.HBM(array.shape, array.dtype),
        scratch_shapes=[pltpu.SemaphoreType.DMA(())],
        compiler_params=pltpu.CompilerParams(vmem_limit_bytes=ADD_LIMIT),
        name="store",
    )(in_vmem(array))


def piece_sizes(width, blocks):
    sizes = [width >> (s + 1) for s in range(blocks.bit_length() - 1)]
    return sizes + sizes[-1:]


def piece_shapes(width, blocks, columns):
    return [pltpu.VMEM((2, size, columns), jnp.bfloat16) for size in piece_sizes(width, blocks)]


def chunk_weights(flat, key_flat, value_flat, blocks, start, count):
    vmem = pl.BlockSpec(memory_space=pltpu.VMEM)
    shapes = piece_shapes(flat.shape[0], blocks, count * DN)
    return pl.pallas_call(
        functools.partial(weights_body, start=start * DN),
        in_specs=[vmem] * 3,
        out_specs=[vmem] * len(shapes),
        out_shape=shapes,
        compiler_params=pltpu.CompilerParams(vmem_limit_bytes=VMEM_LIMIT),
        name="weights",
    )(*[in_vmem(a) for a in (flat, key_flat, value_flat)])


def in_vmem(array):
    return pltpu.with_memory_space_constraint(array, pltpu.VMEM)


def load(place, positions, order, latent, rope, query, grad_out, attn_out, lse, w_uk, w_uv):
    ctx_size = positions.shape[0]
    rows, width = latent.shape
    flat_size = w_uk.shape[1]
    like = lambda a: pltpu.VMEM(a.shape, a.dtype)
    vmem = pl.BlockSpec(memory_space=pltpu.VMEM)
    operands = [positions, order, latent, rope, query, grad_out, attn_out, lse, w_uk, w_uv]
    operands = [pltpu.with_memory_space_constraint(a, pltpu.HBM) for a in operands]
    outs = [like(a) for a in (latent, rope, query, grad_out, lse, lse, w_uk, w_uv)]
    outs += [pltpu.VMEM((rows, flat_size), jnp.bfloat16)] * 2
    outs += [pltpu.VMEM((width, rows), jnp.bfloat16), pltpu.VMEM((ctx_size * rows, rows), jnp.float32)]
    return pl.pallas_call(
        functools.partial(load_body, ctx_size=ctx_size),
        in_specs=[pl.BlockSpec(memory_space=pltpu.SMEM)]
        + [pl.BlockSpec(memory_space=pltpu.HBM)] * len(operands),
        out_specs=[vmem] * len(outs),
        out_shape=outs,
        scratch_shapes=[like(positions), like(order), like(attn_out), pltpu.SemaphoreType.DMA((10,))],
        compiler_params=pltpu.CompilerParams(vmem_limit_bytes=LOAD_LIMIT),
        name="load",
    )(place, *operands)


def all_grads(place, order, latents, ropes, loaded):
    ctx_size = len(latents) + 1
    rows, width = loaded[0].shape
    head_count = loaded[4].shape[0]
    spread = pltpu.VMEM((ctx_size * rows, head_count * DN), jnp.bfloat16)
    total = pltpu.VMEM((rows + DR * rows // width, width), jnp.bfloat16)
    flat = pltpu.VMEM((width, ctx_size * rows), jnp.bfloat16)
    operands = [in_vmem(a) for a in (order, *latents, *ropes, *loaded)]
    vmem = pl.BlockSpec(memory_space=pltpu.VMEM)
    outs = pl.pallas_call(
        functools.partial(grads_body, ctx_size=ctx_size, group=math.gcd(head_count, GROUP)),
        in_specs=[pl.BlockSpec(memory_space=pltpu.SMEM)] + [vmem] * len(operands),
        out_specs=[vmem] * (4 + ctx_size),
        out_shape=[pltpu.VMEM(loaded[2].shape, jnp.bfloat16), spread, spread, flat]
        + [total] * ctx_size,
        compiler_params=pltpu.CompilerParams(vmem_limit_bytes=LIMIT_A_TOKEN * ctx_size * rows),
        name="grads",
    )(place, *operands)
    return outs[0], outs[1], outs[2], outs[3], outs[4:]


def piece_sum(refs, offsets, size):
    total = refs[0][...].astype(jnp.float32)
    for ref, first in zip(refs[1:], offsets):
        total = total + ref[:, first:first + size, :].astype(jnp.float32)
    return total.astype(jnp.bfloat16)


def add_body(*refs, offsets):
    refs[-1][...] = piece_sum(refs[:-1], offsets, refs[0].shape[1])


def finish_body(mine_ref, other_ref, latent_out, rope_out):
    rows = latent_out.shape[0]
    total = mine_ref[...].astype(jnp.float32) + other_ref[...].astype(jnp.float32)
    latent_out[...] = total[:rows]
    extra = total.shape[0] - rows
    for k in range(rope_out.shape[0] // extra):
        rope_out[k * extra:(k + 1) * extra, :] = total[rows:, k * rows:(k + 1) * rows]


def finish(mine, other, rows):
    width = mine.shape[1]
    vmem = pl.BlockSpec(memory_space=pltpu.VMEM)
    return pl.pallas_call(
        finish_body,
        in_specs=[vmem] * 2,
        out_specs=[vmem] * 2,
        out_shape=[jax.ShapeDtypeStruct((rows, width), jnp.float32),
                   jax.ShapeDtypeStruct((DR, rows), jnp.float32)],
        compiler_params=pltpu.CompilerParams(vmem_limit_bytes=ADD_LIMIT),
        name="finish",
    )(in_vmem(mine), in_vmem(other))


def last_body(*refs):
    *refs, uk_ref, uv_ref = refs
    first = 0
    for keep_ref, arrival_ref in zip(refs[::2], refs[1::2]):
        total = piece_sum((keep_ref, arrival_ref), (0,), keep_ref.shape[1])
        width = keep_ref.shape[2]
        uk_ref[:, first:first + width] = total[0]
        uv_ref[:, first:first + width] = total[1]
        first += width


def piece_offsets(pieces, stage):
    sizes = [p.shape[1] for p in pieces]
    return tuple(sum(sizes[past + 1:stage]) for past in range(stage))


def add_arrivals(pieces, stage, arrivals):
    operands = [in_vmem(a) for a in (pieces[stage], *arrivals)]
    vmem = pl.BlockSpec(memory_space=pltpu.VMEM)
    return pl.pallas_call(
        functools.partial(add_body, offsets=piece_offsets(pieces, stage)),
        in_specs=[vmem] * len(operands),
        out_specs=vmem,
        out_shape=pltpu.VMEM(pieces[stage].shape, jnp.bfloat16),
        compiler_params=pltpu.CompilerParams(vmem_limit_bytes=ADD_LIMIT),
        name="add",
    )(*operands)


def last_sums(keeps, arrivals):
    operands = [in_vmem(a) for pair in zip(keeps, arrivals) for a in pair]
    size = keeps[0].shape[1]
    vmem = pl.BlockSpec(memory_space=pltpu.VMEM)
    out = jax.ShapeDtypeStruct((size, sum(k.shape[2] for k in keeps)), jnp.bfloat16)
    return pl.pallas_call(
        last_body,
        in_specs=[vmem] * len(operands),
        out_specs=[vmem] * 2,
        out_shape=[out, out],
        compiler_params=pltpu.CompilerParams(vmem_limit_bytes=ADD_LIMIT),
        name="last",
    )(*operands)


def shifted(value, axis, steps):
    count = lax.axis_size(axis)
    return lax.ppermute(value, axis, [(s, (s + steps) % count) for s in range(count)])


def on_device(latent, rope, query, grad_out, attn_out, lse, positions, w_uk, w_uv):
    dp_size, ctx_size, head_size = (lax.axis_size(a) for a in ("dp", "ctx", "head"))
    rows, width = latent.shape[1:]
    my_ctx = lax.axis_index("ctx")
    my_place = lax.axis_index("dp") * ctx_size + my_ctx
    place = jnp.stack([my_place, my_ctx]).astype(jnp.int32)
    order = jnp.asarray(row_table(dp_size, ctx_size, width))[:, None, :]
    rope_cols = rope[0].T
    latents = [shifted(latent[0], "ctx", -s) for s in range(1, ctx_size)]
    ropes = [shifted(rope_cols, "ctx", -s) for s in range(1, ctx_size)]
    loaded = load(place, positions.reshape(ctx_size, 1, rows), order, latent[0], rope_cols, query[0],
                  grad_out[0], attn_out[0], lse[0], w_uk, w_uv)
    query_grad, key_flat, value_flat, flat, totals = all_grads(place, order, latents, ropes, loaded)
    head_count = lse.shape[1]
    quarter = head_count // 4
    last = quarter // 2
    counts = [quarter, head_count - quarter - last, last] if last else [head_count]
    chunk_pieces = []
    for chunk, count in enumerate(counts):
        chunk_pieces.append(chunk_weights(flat, key_flat, value_flat, dp_size * ctx_size,
                                          sum(counts[:chunk]), count))
    query_grad = store(query_grad)
    summed = totals[0].astype(jnp.float32)
    for s in range(1, ctx_size):
        summed = summed + shifted(totals[s], "ctx", s).astype(jnp.float32)
    mine, other = summed.astype(jnp.bfloat16), jnp.zeros(summed.shape, jnp.bfloat16)
    for bit in bits_of(head_size):
        mine = summed.astype(jnp.bfloat16)
        other = lax.ppermute(mine, "head", [(s, s ^ bit) for s in range(head_size)])
        summed = mine.astype(jnp.float32) + other.astype(jnp.float32)
    grad_latent, grad_rope = finish(mine, other, rows)
    keeps = []
    lasts = []
    for pieces in chunk_pieces:
        arrivals = []
        for stage in range(len(pieces) - 1):
            value = add_arrivals(pieces, stage, arrivals) if stage else pieces[0]
            pairs = stage_pairs(stage, dp_size, ctx_size)
            arrivals.append(lax.ppermute(value, ("dp", "ctx"), pairs))
        keeps.append(add_arrivals(pieces, len(pieces) - 1, arrivals[:-1]))
        lasts.append(arrivals[-1])
    weight_uk, weight_uv = last_sums(keeps, lasts)
    return (
        query_grad[None],
        grad_latent[None],
        grad_rope.T[None],
        weight_uk,
        weight_uv,
    )


def solution(mesh):
    return jax.shard_map(
        on_device,
        mesh=mesh,
        in_specs=(
            P("dp", "ctx", None),
            P("dp", "ctx", None),
            P("dp", "ctx", "head"),
            P("dp", "ctx", "head"),
            P("dp", "ctx", "head"),
            P("dp", "head", "ctx"),
            P("dp", None),
            P(None, "head"),
            P(None, "head"),
        ),
        out_specs=(
            P("dp", "ctx", "head"),
            P("dp", "ctx", None),
            P("dp", "ctx", None),
            P(("dp", "ctx"), "head"),
            P(("dp", "ctx"), "head"),
        ),
        check_vma=False,
    )
```

```python
import functools
import math

import jax
import jax.numpy as jnp
import numpy as np
from jax import lax
from jax.experimental import pallas as pl
from jax.experimental.pallas import tpu as pltpu
from jax.sharding import PartitionSpec as P


DR = 64
DN = 128
DV = 128
DQ = DN + DR

MASKED = -1e30
GROUP = 16
VMEM_LIMIT = 6 << 20
LIMIT_A_TOKEN = 4 << 10
LOAD_LIMIT = 4 << 20
ADD_LIMIT = 2 << 20
NT = (((1,), (1,)), ((), ()))


def bits_of(count):
    return [1 << b for b in range(count.bit_length() - 1)]


def stage_orders(dp_size, ctx_size):
    outer = [("dp", bit) for bit in bits_of(dp_size)[1:]]
    inner = [("ctx", bit) for bit in bits_of(ctx_size)]
    return outer + inner, inner + outer


def row_table(dp_size, ctx_size, rows):
    orders = stage_orders(dp_size, ctx_size)
    blocks = dp_size * ctx_size
    width = rows // blocks
    table = np.zeros((blocks, rows), np.int32)
    for dp in range(dp_size):
        for ctx in range(ctx_size):
            for place in range(blocks):
                digits = [(place >> b) & 1 for b in reversed(range(blocks.bit_length() - 1))]
                target = {"dp": dp, "ctx": ctx}
                if digits[0] == 0:
                    target["dp"] ^= 1
                for digit, (axis, bit) in zip(digits[1:], orders[target["dp"] & 1]):
                    if digit == 0:
                        target[axis] ^= bit
                block = target["dp"] * ctx_size + target["ctx"]
                table[dp * ctx_size + ctx, place * width:(place + 1) * width] = (
                    block * width + np.arange(width)
                )
    return table


def stage_pairs(stage, dp_size, ctx_size):
    pairs = []
    orders = stage_orders(dp_size, ctx_size)
    for dp in range(dp_size):
        for ctx in range(ctx_size):
            place = {"dp": dp, "ctx": ctx}
            axis, bit = ("dp", 1) if stage == 0 else orders[dp & 1][stage - 1]
            place[axis] ^= bit
            pairs.append((dp * ctx_size + ctx, place["dp"] * ctx_size + place["ctx"]))
    return pairs


def dot(a, b):
    return jnp.dot(a, b, preferred_element_type=jnp.float32)


def dot_nt(a, b):
    return lax.dot_general(a, b, NT, preferred_element_type=jnp.float32)


def load_body(place_ref, pos_ref, order_ref, latent_ref, rope_ref, query_ref, grad_ref, out_ref,
              lse_ref, wuk_ref, wuv_ref, latent_out, rope_out, query_out, grad_out, lse_out,
              delta_out, wuk_out, wuv_out, keys_out, values_out, flat_out, bias_out,
              pos, order, attn, sems, *, ctx_size):
    pairs = [(latent_ref, latent_out), (order_ref, order), (pos_ref, pos), (grad_ref, grad_out),
             (out_ref, attn), (wuk_ref, wuk_out), (wuv_ref, wuv_out), (query_ref, query_out),
             (rope_ref, rope_out), (lse_ref, lse_out)]
    copies = [pltpu.make_async_copy(a, b, sems.at[k]) for k, (a, b) in enumerate(pairs)]
    for copy in copies:
        copy.start()
    rows, _ = latent_out.shape
    for copy in copies[:3]:
        copy.wait()
    mine = place_ref[1]
    own_pos = jnp.broadcast_to(pos[mine], (rows, rows))
    for chunk in range(ctx_size):
        key_pos = pos[lax.rem(mine + chunk, ctx_size)]
        key_col = jnp.broadcast_to(key_pos, (rows, rows)).T
        bias_out[chunk * rows:(chunk + 1) * rows, :] = jnp.where(key_col <= own_pos, 0.0, MASKED)
    latent = latent_out[...]
    flat_out[...] = rows_first(latent, order[place_ref[0]])
    copies[3].wait()
    copies[4].wait()
    for head in range(delta_out.shape[0]):
        cols = slice(head * DV, (head + 1) * DV)
        product = grad_out[:, cols].astype(jnp.float32) * attn[:, cols].astype(jnp.float32)
        delta_out[head:head + 1, :] = jnp.sum(product.T, axis=0, keepdims=True)
    copies[5].wait()
    keys_out[...] = dot(latent, wuk_out[...]).astype(jnp.bfloat16)
    copies[6].wait()
    values_out[...] = dot(latent, wuv_out[...]).astype(jnp.bfloat16)
    for copy in copies[7:]:
        copy.wait()


def rows_first(latent, order):
    width = latent.shape[1]
    spot = lax.broadcasted_iota(jnp.int32, (width, width), 0)
    pick = jnp.where(spot == order, 1.0, 0.0).astype(jnp.bfloat16)
    return dot(latent, pick).astype(jnp.bfloat16).T


def grads_body(place_ref, order_ref, *rest, ctx_size, group):
    far_latents = rest[:ctx_size - 1]
    far_ropes = rest[ctx_size - 1:2 * ctx_size - 2]
    (latent_ref, rope_ref, query_ref, grad_ref, lse_ref, delta_ref, wuk_ref, wuv_ref, keys_ref,
     values_ref, flat_ref, bias_ref, *rest) = rest[2 * ctx_size - 2:]
    dq_ref, key_out, value_out, flat_out, *total_refs = rest
    rows, _ = latent_ref.shape
    scale = 1.0 / math.sqrt(DQ)
    rope = jnp.concatenate([ref[...] for ref in (rope_ref, *far_ropes)], axis=1).T
    far = jnp.concatenate([ref[...] for ref in far_latents], axis=0)
    bias = bias_ref[...]
    flat_out[...] = jnp.concatenate(
        [flat_ref[...], rows_first(far, order_ref[place_ref[0]])], axis=1
    )
    rope_total = 0.0
    latent_total = 0.0
    for first in range(0, lse_ref.shape[0], group):
        span = slice(first * DN, (first + group) * DN)
        wuk = wuk_ref[:, span]
        wuv = wuv_ref[:, span]
        keys_all = jnp.concatenate([keys_ref[:, span], dot(far, wuk).astype(jnp.bfloat16)], axis=0)
        values_all = jnp.concatenate(
            [values_ref[:, span], dot(far, wuv).astype(jnp.bfloat16)], axis=0
        )
        key_grads = []
        value_grads = []
        stages = []
        for inner in range(group + 2):
            if inner < group:
                head = first + inner
                cols = slice(head * DN, (head + 1) * DN)
                wide = slice(head * DQ, (head + 1) * DQ)
                part = slice(inner * DN, (inner + 1) * DN)
                keys = jnp.concatenate([keys_all[:, part], rope], axis=1)
                query = query_ref[:, wide]
                grad = grad_ref[:, cols]
                stages.append([head, wide, keys, query, grad, dot_nt(keys, query),
                               dot_nt(values_all[:, part], grad)])
            if 0 <= inner - 2:
                wide, keys, query, grad, score_grad, weights_b = stages[inner - 2]
                dq_ref[:, wide] = dot(score_grad.T, keys).astype(jnp.bfloat16)
                key_grad = dot(score_grad, query)
                value_grads.append(dot(weights_b, grad).astype(jnp.bfloat16))
                key_grads.append(key_grad[:, :DN].astype(jnp.bfloat16))
                rope_total = rope_total + key_grad[:, DN:]
            if 0 <= inner - 1 < group:
                head, wide, keys, query, grad, scores, dots = stages[inner - 1]
                weights = jnp.exp(scores * scale - lse_ref[head:head + 1, :] + bias)
                score_grad = weights * (dots - delta_ref[head:head + 1, :]) * scale
                stages[inner - 1] = (wide, keys, query, grad, score_grad.astype(jnp.bfloat16),
                                     weights.astype(jnp.bfloat16))
        key_flat = jnp.concatenate(key_grads, axis=1)
        value_flat = jnp.concatenate(value_grads, axis=1)
        key_out[:, span] = key_flat
        value_out[:, span] = value_flat
        latent_total = latent_total + dot_nt(key_flat, wuk) + dot_nt(value_flat, wuv)
    for chunk, total_ref in enumerate(total_refs):
        part = slice(chunk * rows, (chunk + 1) * rows)
        total_ref[:rows, :] = latent_total[part].astype(jnp.bfloat16)
        rope_cols = rope_total[part].T.astype(jnp.bfloat16)
        extra = total_ref.shape[0] - rows
        for k in range(DR // extra):
            total_ref[rows:, k * rows:(k + 1) * rows] = rope_cols[k * extra:(k + 1) * extra]


def write_pieces(piece_refs, span, flat, key_flat, value_flat):
    row = 0
    for piece_ref in piece_refs:
        size = piece_ref.shape[1]
        piece_ref[0, :, span] = dot(flat[row:row + size], key_flat).astype(jnp.bfloat16)
        piece_ref[1, :, span] = dot(flat[row:row + size], value_flat).astype(jnp.bfloat16)
        row += size


def weights_body(flat_ref, key_ref, value_ref, *piece_refs, start):
    flat = flat_ref[...]
    count = piece_refs[0].shape[2]
    step = math.gcd(count, 256)
    for first in range(0, count, step):
        part = slice(start + first, start + first + step)
        span = slice(first, first + step)
        write_pieces(piece_refs, span, flat, key_ref[:, part], value_ref[:, part])


def store_body(source_ref, out_ref, sem):
    copy = pltpu.make_async_copy(source_ref, out_ref, sem)
    copy.start()
    copy.wait()


def store(array):
    return pl.pallas_call(
        store_body,
        in_specs=[pl.BlockSpec(memory_space=pltpu.VMEM)],
        out_specs=pl.BlockSpec(memory_space=pltpu.HBM),
        out_shape=pltpu.HBM(array.shape, array.dtype),
        scratch_shapes=[pltpu.SemaphoreType.DMA(())],
        compiler_params=pltpu.CompilerParams(vmem_limit_bytes=ADD_LIMIT),
        name="store",
    )(in_vmem(array))


def piece_sizes(width, blocks):
    sizes = [width >> (s + 1) for s in range(blocks.bit_length() - 1)]
    return sizes + sizes[-1:]


def piece_shapes(width, blocks, columns):
    return [pltpu.VMEM((2, size, columns), jnp.bfloat16) for size in piece_sizes(width, blocks)]


def chunk_weights(flat, key_flat, value_flat, blocks, start, count):
    vmem = pl.BlockSpec(memory_space=pltpu.VMEM)
    shapes = piece_shapes(flat.shape[0], blocks, count * DN)
    return pl.pallas_call(
        functools.partial(weights_body, start=start * DN),
        in_specs=[vmem] * 3,
        out_specs=[vmem] * len(shapes),
        out_shape=shapes,
        compiler_params=pltpu.CompilerParams(vmem_limit_bytes=VMEM_LIMIT),
        name="weights",
    )(*[in_vmem(a) for a in (flat, key_flat, value_flat)])


def in_vmem(array):
    return pltpu.with_memory_space_constraint(array, pltpu.VMEM)


def load(place, positions, order, latent, rope, query, grad_out, attn_out, lse, w_uk, w_uv):
    ctx_size = positions.shape[0]
    rows, width = latent.shape
    flat_size = w_uk.shape[1]
    like = lambda a: pltpu.VMEM(a.shape, a.dtype)
    vmem = pl.BlockSpec(memory_space=pltpu.VMEM)
    operands = [positions, order, latent, rope, query, grad_out, attn_out, lse, w_uk, w_uv]
    operands = [pltpu.with_memory_space_constraint(a, pltpu.HBM) for a in operands]
    outs = [like(a) for a in (latent, rope, query, grad_out, lse, lse, w_uk, w_uv)]
    outs += [pltpu.VMEM((rows, flat_size), jnp.bfloat16)] * 2
    outs += [pltpu.VMEM((width, rows), jnp.bfloat16), pltpu.VMEM((ctx_size * rows, rows), jnp.float32)]
    return pl.pallas_call(
        functools.partial(load_body, ctx_size=ctx_size),
        in_specs=[pl.BlockSpec(memory_space=pltpu.SMEM)]
        + [pl.BlockSpec(memory_space=pltpu.HBM)] * len(operands),
        out_specs=[vmem] * len(outs),
        out_shape=outs,
        scratch_shapes=[like(positions), like(order), like(attn_out), pltpu.SemaphoreType.DMA((10,))],
        compiler_params=pltpu.CompilerParams(vmem_limit_bytes=LOAD_LIMIT),
        name="load",
    )(place, *operands)


def all_grads(place, order, latents, ropes, loaded):
    ctx_size = len(latents) + 1
    rows, width = loaded[0].shape
    head_count = loaded[4].shape[0]
    spread = pltpu.VMEM((ctx_size * rows, head_count * DN), jnp.bfloat16)
    total = pltpu.VMEM((rows + DR * rows // width, width), jnp.bfloat16)
    flat = pltpu.VMEM((width, ctx_size * rows), jnp.bfloat16)
    operands = [in_vmem(a) for a in (order, *latents, *ropes, *loaded)]
    vmem = pl.BlockSpec(memory_space=pltpu.VMEM)
    outs = pl.pallas_call(
        functools.partial(grads_body, ctx_size=ctx_size, group=math.gcd(head_count, GROUP)),
        in_specs=[pl.BlockSpec(memory_space=pltpu.SMEM)] + [vmem] * len(operands),
        out_specs=[vmem] * (4 + ctx_size),
        out_shape=[pltpu.VMEM(loaded[2].shape, jnp.bfloat16), spread, spread, flat]
        + [total] * ctx_size,
        compiler_params=pltpu.CompilerParams(vmem_limit_bytes=LIMIT_A_TOKEN * ctx_size * rows * head_count),
        name="grads",
    )(place, *operands)
    return outs[0], outs[1], outs[2], outs[3], outs[4:]


def piece_sum(refs, offsets, size):
    total = refs[0][...].astype(jnp.float32)
    for ref, first in zip(refs[1:], offsets):
        total = total + ref[:, first:first + size, :].astype(jnp.float32)
    return total.astype(jnp.bfloat16)


def add_body(*refs, offsets):
    refs[-1][...] = piece_sum(refs[:-1], offsets, refs[0].shape[1])


def finish_body(mine_ref, other_ref, latent_out, rope_out):
    rows = latent_out.shape[0]
    total = mine_ref[...].astype(jnp.float32) + other_ref[...].astype(jnp.float32)
    latent_out[...] = total[:rows]
    extra = total.shape[0] - rows
    for k in range(rope_out.shape[0] // extra):
        rope_out[k * extra:(k + 1) * extra, :] = total[rows:, k * rows:(k + 1) * rows]


def finish(mine, other, rows):
    width = mine.shape[1]
    vmem = pl.BlockSpec(memory_space=pltpu.VMEM)
    return pl.pallas_call(
        finish_body,
        in_specs=[vmem] * 2,
        out_specs=[vmem] * 2,
        out_shape=[jax.ShapeDtypeStruct((rows, width), jnp.float32),
                   jax.ShapeDtypeStruct((DR, rows), jnp.float32)],
        compiler_params=pltpu.CompilerParams(vmem_limit_bytes=ADD_LIMIT),
        name="finish",
    )(in_vmem(mine), in_vmem(other))


def last_body(*refs):
    *refs, uk_ref, uv_ref = refs
    first = 0
    for keep_ref, arrival_ref in zip(refs[::2], refs[1::2]):
        total = piece_sum((keep_ref, arrival_ref), (0,), keep_ref.shape[1])
        width = keep_ref.shape[2]
        uk_ref[:, first:first + width] = total[0]
        uv_ref[:, first:first + width] = total[1]
        first += width


def piece_offsets(pieces, stage):
    sizes = [p.shape[1] for p in pieces]
    return tuple(sum(sizes[past + 1:stage]) for past in range(stage))


def add_arrivals(pieces, stage, arrivals):
    operands = [in_vmem(a) for a in (pieces[stage], *arrivals)]
    vmem = pl.BlockSpec(memory_space=pltpu.VMEM)
    return pl.pallas_call(
        functools.partial(add_body, offsets=piece_offsets(pieces, stage)),
        in_specs=[vmem] * len(operands),
        out_specs=vmem,
        out_shape=pltpu.VMEM(pieces[stage].shape, jnp.bfloat16),
        compiler_params=pltpu.CompilerParams(vmem_limit_bytes=ADD_LIMIT),
        name="add",
    )(*operands)


def last_sums(keeps, arrivals):
    operands = [in_vmem(a) for pair in zip(keeps, arrivals) for a in pair]
    size = keeps[0].shape[1]
    vmem = pl.BlockSpec(memory_space=pltpu.VMEM)
    out = jax.ShapeDtypeStruct((size, sum(k.shape[2] for k in keeps)), jnp.bfloat16)
    return pl.pallas_call(
        last_body,
        in_specs=[vmem] * len(operands),
        out_specs=[vmem] * 2,
        out_shape=[out, out],
        compiler_params=pltpu.CompilerParams(vmem_limit_bytes=ADD_LIMIT),
        name="last",
    )(*operands)


def shifted(value, axis, steps):
    count = lax.axis_size(axis)
    return lax.ppermute(value, axis, [(s, (s + steps) % count) for s in range(count)])


def on_device(latent, rope, query, grad_out, attn_out, lse, positions, w_uk, w_uv):
    dp_size, ctx_size, head_size = (lax.axis_size(a) for a in ("dp", "ctx", "head"))
    rows, width = latent.shape[1:]
    my_ctx = lax.axis_index("ctx")
    my_place = lax.axis_index("dp") * ctx_size + my_ctx
    place = jnp.stack([my_place, my_ctx]).astype(jnp.int32)
    order = jnp.asarray(row_table(dp_size, ctx_size, width))[:, None, :]
    rope_cols = rope[0].T
    latents = [shifted(latent[0], "ctx", -s) for s in range(1, ctx_size)]
    ropes = [shifted(rope_cols, "ctx", -s) for s in range(1, ctx_size)]
    loaded = load(place, positions.reshape(ctx_size, 1, rows), order, latent[0], rope_cols, query[0],
                  grad_out[0], attn_out[0], lse[0], w_uk, w_uv)
    query_grad, key_flat, value_flat, flat, totals = all_grads(place, order, latents, ropes, loaded)
    head_count = lse.shape[1]
    quarter = head_count // 4
    last = quarter // 2
    last += last // 2
    counts = [quarter, head_count - quarter - last, last] if last else [head_count]
    chunk_pieces = []
    for chunk, count in enumerate(counts):
        chunk_pieces.append(chunk_weights(flat, key_flat, value_flat, dp_size * ctx_size,
                                          sum(counts[:chunk]), count))
    query_grad = store(query_grad)
    summed = totals[0].astype(jnp.float32)
    for s in range(1, ctx_size):
        summed = summed + shifted(totals[s], "ctx", s).astype(jnp.float32)
    mine, other = summed.astype(jnp.bfloat16), jnp.zeros(summed.shape, jnp.bfloat16)
    for bit in bits_of(head_size):
        mine = summed.astype(jnp.bfloat16)
        other = lax.ppermute(mine, "head", [(s, s ^ bit) for s in range(head_size)])
        summed = mine.astype(jnp.float32) + other.astype(jnp.float32)
    grad_latent, grad_rope = finish(mine, other, rows)
    keeps = []
    lasts = []
    for pieces in chunk_pieces:
        arrivals = []
        for stage in range(len(pieces) - 1):
            value = add_arrivals(pieces, stage, arrivals) if stage else pieces[0]
            pairs = stage_pairs(stage, dp_size, ctx_size)
            arrivals.append(lax.ppermute(value, ("dp", "ctx"), pairs))
        keeps.append(add_arrivals(pieces, len(pieces) - 1, arrivals[:-1]))
        lasts.append(arrivals[-1])
    weight_uk, weight_uv = last_sums(keeps, lasts)
    return (
        query_grad[None],
        grad_latent[None],
        grad_rope.T[None],
        weight_uk,
        weight_uv,
    )


def solution(mesh):
    return jax.shard_map(
        on_device,
        mesh=mesh,
        in_specs=(
            P("dp", "ctx", None),
            P("dp", "ctx", None),
            P("dp", "ctx", "head"),
            P("dp", "ctx", "head"),
            P("dp", "ctx", "head"),
            P("dp", "head", "ctx"),
            P("dp", None),
            P(None, "head"),
            P(None, "head"),
        ),
        out_specs=(
            P("dp", "ctx", "head"),
            P("dp", "ctx", None),
            P("dp", "ctx", None),
            P(("dp", "ctx"), "head"),
            P(("dp", "ctx"), "head"),
        ),
        check_vma=False,
    )
```
